768 devices in a mesh: dp: 96 (over y, x, z_hi), pipe: 8 (over z_lo, core).
Axes of the slice: x: 4, y: 8, z: 12 (z_hi: 3, z_lo: 4; z = z_hi * 4 + z_lo), core: 2. Of those that a mesh axis runs over, the one named last changes fastest.
Arguments:
- embed_grad: bfloat16 [6144, 4608], P('dp', 'pipe'), may hold values from -0.35 to 0.35
- ids: int32 [6144], P('dp'), may hold values from 0 to 135167
Outputs:
- table_grad: float32 [135168, 4608], P('dp', 'pipe')
The draws below stay inside these ranges and needn't reach their ends.
All inputs are finite; a program needn't handle non-finite values.
Results may differ from the reference program's by a relative error of at most 0.00035.
Values may be sent and summed in bfloat16 or wider, within the bound.
No kernel may reach another device: no remote copies, remote signals or barrier semaphores. Data moves between devices by JAX's collectives and lax.ppermute only.
A program may use at most 64 MiB of HBM per device.

```python
import math
import jax
import jax.numpy as jnp
import numpy as np
from jax import lax

D = 4608
VOC_DEV = 1408
TOKENS = 6144
VOCAB = 135168
N_DP = 96


def draw_embed_grad(key, part):
    rows = jnp.arange(TOKENS, dtype=jnp.float32)[:, None] / TOKENS
    columns = jnp.arange(D, dtype=jnp.float32)[None, :] / D
    noise = jnp.clip(jax.random.normal(key, (TOKENS, D), jnp.float32), -5.0, 5.0)
    scale = 0.015 * jnp.exp(jnp.log(3.0) * rows) * jnp.exp(jnp.log(1.5) * columns)
    values = noise * scale
    return jnp.clip(values, -0.35, 0.35).astype(jnp.bfloat16)


def set_ends(drawn, key, low, high):
    longest = drawn.shape.index(max(drawn.shape))
    spots = []
    for shift in (0, 1):
        where = [jax.random.randint(jax.random.fold_in(key, axis), (), 0, length) for axis, length in enumerate(drawn.shape)]
        where[longest] = (where[longest] + shift) % drawn.shape[longest]
        spots.append(tuple(where))
    return drawn.at[spots[0]].set(low).at[spots[1]].set(high)


def skewed_wide(rng, extent, number_of, lean):
    loads = [min(1 << octave, number_of + 1 - (1 << octave)) * (1 << 20) // math.isqrt((1 << octave) ** lean) + 1 for octave in range((number_of + 1).bit_length()) if 1 << octave <= number_of]
    spread = 1 + sum(loads) // (1 << 30)
    listing = np.cumsum(np.array([max(1, weight // spread) for weight in loads]))
    ticket = jax.random.randint(jax.random.fold_in(rng, 1), extent, 0, int(listing[len(loads) - 1]))
    start = jnp.left_shift(1, jnp.searchsorted(jnp.asarray(listing, jnp.int32), ticket, side="right").astype(jnp.int32))
    grade = start - 1 + jax.random.randint(jax.random.fold_in(rng, 4), extent, 0, 1 << 30) % jnp.minimum(start, number_of + 1 - start)
    return jax.random.permutation(jax.random.fold_in(rng, 2), number_of)[grade].astype(jnp.int32)


def setup_inputs(seed: int = 0) -> dict:
    seeds = jax.random.split(jax.random.key(seed), 3)
    return {
        "embed_grad": draw_embed_grad(jax.random.fold_in(seeds[2], 71), 0),
        "ids": set_ends(skewed_wide(seeds[1], (TOKENS,), VOCAB, 2), jax.random.fold_in(seeds[1], 3), 0, VOCAB - 1).astype(jnp.int32),
    }


def reference(embed_grad, ids):
    cotangent = embed_grad.astype(jnp.float32)

    def block_rows(block_index):
        start = block_index * VOC_DEV
        local = ids - start
        inside = (local >= 0) & (local < VOC_DEV)
        segment = jnp.where(inside, local, VOC_DEV).astype(jnp.int32)
        summed = jax.ops.segment_sum(cotangent, segment, VOC_DEV + 1)
        return summed[:VOC_DEV] * math.sqrt(D)
    grad_rows = lax.map(block_rows, jnp.arange(N_DP, dtype=jnp.int32))
    grad_norm = jnp.sqrt(jnp.sum(grad_rows * grad_rows) + 1e-06)
    factor = jnp.minimum(1.0, 0.2 * math.sqrt(TOKENS * D) / grad_norm)
    return (grad_rows * factor).reshape(VOCAB, D)
```

```python
import functools
import math

import jax
import jax.numpy as jnp
from jax import lax
from jax.experimental import pallas as pl
from jax.experimental.pallas import tpu as pltpu
from jax.sharding import Mesh
from jax.sharding import PartitionSpec as P

D = 4608
VOC_DEV = 1408
WIDE = 640
TAIL = 512
AUX = 64
Y, X, ZH, ZL, CORE = AXES = ("dp_0", "dp_1", "dp_2", "pipe_0", "pipe_1")
DP = AXES[:3]
PIPE = AXES[3:]
F32 = jnp.float32
BF16 = jnp.bfloat16

FIRST = (ZH,)
FIRST_CAP = 48
SECOND = (Y, X)
SECOND_CAP = 16
NORM_1 = (Y, X, CORE)
NORM_2 = (ZH, ZL)


def axis_size(axes):
    return math.prod({Y: 8, X: 4, ZH: 3, ZL: 4, CORE: 2}[a] for a in axes)


def floor_div(value, by):
    return jnp.floor((value + 0.5) * (1.0 / by))


def place(code, axes):
    y = floor_div(code - 1.0, 12 * VOC_DEV)
    rest = code - 1.0 - y * (12 * VOC_DEV)
    x = floor_div(rest, 3 * VOC_DEV)
    zh = floor_div(rest - x * (3 * VOC_DEV), VOC_DEV)
    index = 0.0
    for axis in axes:
        index = index * axis_size((axis,)) + {Y: y, X: x, ZH: zh}[axis]
    return index


def square_iota(n):
    return (lax.broadcasted_iota(jnp.int32, (n, n), 0), lax.broadcasted_iota(jnp.int32, (n, n), 1))


def column_to_row(column):
    i, j = square_iota(column.shape[0])
    return jnp.sum(jnp.where(i == j, column, 0.0), axis=0, keepdims=True)


def row_to_column(row):
    i, j = square_iota(row.shape[1])
    return jnp.sum(jnp.where(i == j, row, 0.0), axis=1, keepdims=True)


def decode(tail):
    lane = lax.broadcasted_iota(jnp.int32, (1, 128), 1)
    weight = jnp.where(lane == AUX, 1024.0, jnp.where(lane == AUX + 1, 8.0, jnp.where(lane == AUX + 2, 1.0, 0.0)))
    return jnp.sum(tail.astype(F32) * weight, axis=1, keepdims=True)


def encode(code):
    high = jnp.floor(code * (1.0 / 1024))
    rest = code - high * 1024.0
    middle = jnp.floor(rest * (1.0 / 8))
    low = rest - middle * 8.0
    lane = lax.broadcasted_iota(jnp.int32, (1, 128), 1)
    return jnp.where(lane == AUX, high, jnp.where(lane == AUX + 1, middle, jnp.where(lane == AUX + 2, low, 0.0)))


def pack(code_row, code_col, axes, cap):
    n = code_row.shape[1]
    i, j = square_iota(n)
    real_row = code_row > 0.5
    real_col = code_col > 0.5
    to_row = jnp.where(real_row, place(code_row, axes), -1.0)
    to_col = jnp.where(real_col, place(code_col, axes), -1.0)
    same = jnp.where((code_col == code_row) & real_row, 1.0, 0.0)
    above = jnp.where(i < j, same, 0.0)
    below = jnp.where(j < i, same, 0.0)
    count_row = jnp.sum(same, axis=0, keepdims=True)
    lead_row = (jnp.sum(above, axis=0, keepdims=True) == 0.0) & real_row
    lead_col = (jnp.sum(below, axis=1, keepdims=True) == 0.0) & real_col
    width_row = jnp.where(lead_row, jnp.minimum(count_row, 2.0), 0.0)
    before = jnp.sum(jnp.where((to_col == to_row) & (j < i), width_row, 0.0), axis=1, keepdims=True)
    before = jnp.where(lead_col, before, 0.0)
    slot_in = jnp.sum(same * before, axis=0, keepdims=True)
    over = jnp.max(jnp.where(real_row & (slot_in + jnp.minimum(count_row, 2.0) > cap), 1.0, 0.0), axis=1, keepdims=True)
    base = jnp.where(real_row, to_row * cap + slot_in, -2.0)
    return base, count_row, lead_row, over


def fill(out_ref, base, count_row, lead_row, code_row, head, tail, slots):
    n = base.shape[1]
    slot = lax.broadcasted_iota(jnp.int32, (slots, n), 0).astype(F32)
    first = slot == base
    second = (slot == base + 1.0) & (count_row > 1.5)
    take = jnp.where(first | second, 1.0, 0.0)
    code = jnp.sum(jnp.where(lead_row, take * code_row, 0.0), axis=1, keepdims=True)
    is_second = jnp.max(jnp.where(second, 1.0, 0.0), axis=1, keepdims=True) > 0.5
    take = take.astype(BF16)

    def split(rows):
        total = jnp.dot(take, rows, preferred_element_type=F32)
        kept = total.astype(BF16).astype(F32)
        return jnp.where(is_second, total - kept, kept)

    out_ref[:, :TAIL] = split(head).astype(BF16)
    lane = lax.broadcasted_iota(jnp.int32, (1, 128), 1)
    out_ref[:, TAIL:] = jnp.where(lane < AUX, split(tail), encode(code)).astype(BF16)


def first_kernel(grad_ref, ids_ref, out_ref, over_ref):
    code_row = ids_ref[...].astype(F32) + 1.0
    code_col = row_to_column(code_row)
    slots = out_ref.shape[0]
    base, count, lead, over = pack(code_row, code_col, FIRST, FIRST_CAP)
    tail = grad_ref[:, TAIL:]
    tail = jnp.concatenate([tail, jnp.zeros_like(tail)], axis=1)
    fill(out_ref, base, count, lead, code_row, grad_ref[:, :TAIL], tail, slots)
    over_ref[...] = jnp.broadcast_to(over, over_ref.shape)


def second_kernel(rows_ref, over_in_ref, out_ref, over_ref):
    tail = rows_ref[:, TAIL:]
    code_col = decode(tail)
    code_row = column_to_row(code_col)
    base, count, lead, over = pack(code_row, code_col, SECOND, SECOND_CAP)
    fill(out_ref, base, count, lead, code_row, rows_ref[:, :TAIL], tail, out_ref.shape[0])
    over_ref[...] = jnp.broadcast_to(over, over_ref.shape) + over_in_ref[...]


def features(rows_ref):
    lane = lax.broadcasted_iota(jnp.int32, (1, 128), 1)
    tail = rows_ref[:, TAIL:]
    return rows_ref[:, :TAIL], jnp.where(lane < AUX, tail.astype(F32), 0.0).astype(BF16)


def norm_kernel(rows_ref, over_ref, part_ref):
    code_col = decode(rows_ref[:, TAIL:])
    code_row = column_to_row(code_col)
    head, tail = features(rows_ref)
    nt = (((1,), (1,)), ((), ()))
    gram = lax.dot_general(head, head, nt, preferred_element_type=F32)
    gram = gram + lax.dot_general(tail, tail, nt, preferred_element_type=F32)
    gram = jnp.where((code_col == code_row) & (code_row > 0.5), gram, 0.0)
    squares = jnp.sum(jnp.sum(gram, axis=0, keepdims=True), axis=1, keepdims=True)
    lane = lax.broadcasted_iota(jnp.int32, (1, 128), 1)
    part = jnp.where(lane == 0, squares, jnp.where(lane == 1, over_ref[:1, :], 0.0))
    part_ref[...] = jnp.broadcast_to(part[:, None, :], part_ref.shape)


def clip_factor(total, tokens):
    grad_norm = jnp.sqrt(total * float(D) + 1e-06)
    return jnp.minimum(1.0, 0.2 * math.sqrt(tokens * D) / grad_norm)


BLOCK = 384


def write_kernel(rows_ref, parts_ref, out_ref, turned_ref, *, tokens):
    @pl.when(pl.program_id(0) == 0)
    def _():
        turned_ref[...] = rows_ref[...].T

    lane = lax.broadcasted_iota(jnp.int32, (1, 128), 1)
    total = jnp.sum(parts_ref[...], axis=0)
    total = jnp.sum(jnp.where(lane == 0, total, 0.0), axis=1, keepdims=True)
    scale = clip_factor(total, tokens) * math.sqrt(D)
    code = decode(rows_ref[:, TAIL:])
    local = code - 1.0
    local = jnp.where(code > 0.5, local - VOC_DEV * floor_div(local, VOC_DEV), -1.0)
    here = lax.broadcasted_iota(jnp.int32, (local.shape[0], BLOCK), 1) + pl.program_id(0) * BLOCK
    pick = jnp.where(here.astype(F32) == local, 1.0, 0.0).astype(BF16)
    features = out_ref.shape[0]
    out_ref[...] = jnp.dot(turned_ref[:features, :], pick, preferred_element_type=F32) * scale


def shape(rows, cols, dtype=F32):
    return jax.ShapeDtypeStruct((rows, cols), dtype)


def around(axes, sizes, value, body, init):
    if not axes:
        return value, body(value, init)
    axis, n = axes[0], sizes[0]
    ring = [(k, (k + 1) % n) for k in range(n)]

    def step(_, carry):
        held, acc = around(axes[1:], sizes[1:], carry[0], body, carry[1])
        return jax.tree.map(lambda a: lax.ppermute(a, axis, ring), held), acc

    return lax.fori_loop(0, n, step, (value, init))


def general(embed_grad, ids):
    tokens = ids.shape[0]
    offset = lax.axis_index(DP) * VOC_DEV

    def add(held, acc):
        rows, names = held
        here = lax.broadcasted_iota(jnp.int32, (VOC_DEV, tokens), 0)
        pick = (here == (names[0] - offset)[None, :]).astype(BF16)
        return acc + jnp.dot(pick, rows, preferred_element_type=F32)

    names = jnp.broadcast_to(ids[None, :], (8, tokens))
    zeros = jnp.zeros((VOC_DEV, embed_grad.shape[1]), F32)
    _, summed = around(DP, (8, 4, 3), (embed_grad, names), add, zeros)
    total = jnp.sum(summed * summed)
    for axis in AXES:
        total = lax.psum(total, axis)
    return summed * (clip_factor(total, tokens * 96) * math.sqrt(D))


def per_device(embed_grad, ids):
    tokens = ids.shape[0]
    cols = embed_grad.shape[1]
    slots_1 = axis_size(FIRST) * FIRST_CAP
    slots_2 = axis_size(SECOND) * SECOND_CAP
    sent, over = pl.pallas_call(first_kernel, out_shape=(shape(slots_1, WIDE, BF16), shape(8, 128)), name="first")(
        embed_grad, ids.reshape(1, tokens)
    )
    held = lax.all_to_all(sent, FIRST, 0, 0, tiled=True)
    sent, over = pl.pallas_call(second_kernel, out_shape=(shape(slots_2, WIDE, BF16), shape(8, 128)), name="second")(
        held, over
    )
    held = lax.all_to_all(sent, SECOND, 0, 0, tiled=True)
    n1, n2 = axis_size(NORM_1), axis_size(NORM_2)
    part = pl.pallas_call(norm_kernel, out_shape=jax.ShapeDtypeStruct((n1, 1, 128), F32), name="squares")(held, over)
    part = lax.all_to_all(part, NORM_1, 0, 0, tiled=True)
    part = jnp.broadcast_to(jnp.sum(part, axis=0, keepdims=True), (n2, 1, 128))
    part = lax.all_to_all(part, NORM_2, 0, 0, tiled=True)
    overflow = jnp.sum(part[:, 0, 1])

    def routed():
        return pl.pallas_call(
            functools.partial(write_kernel, tokens=tokens * 96),
            grid=(pl.cdiv(VOC_DEV, BLOCK),),
            in_specs=[
                pl.BlockSpec((slots_2, WIDE), lambda b: (0, 0)),
                pl.BlockSpec((n2, 1, 128), lambda b: (0, 0, 0)),
            ],
            out_specs=pl.BlockSpec((cols, BLOCK), lambda b: (0, b)),
            out_shape=shape(cols, VOC_DEV),
            scratch_shapes=[pltpu.VMEM((WIDE, slots_2), BF16)],
            name="rows",
        )(held, part).T

    return lax.cond(overflow > 0.0, lambda: general(embed_grad, ids), routed)


def solution(mesh):
    torus = Mesh(mesh.devices.reshape(8, 4, 3, 4, 2), AXES)
    return jax.shard_map(
        per_device,
        mesh=torus,
        in_specs=(P(DP, PIPE), P(DP)),
        out_specs=P(DP, PIPE),
        check_vma=False,
    )
```

```python
import functools
import math

import jax
import jax.numpy as jnp
from jax import lax
from jax.experimental import pallas as pl
from jax.experimental.pallas import tpu as pltpu
from jax.sharding import Mesh
from jax.sharding import PartitionSpec as P

D = 4608
VOC_DEV = 1408
WIDE = 640
TAIL = 512
AUX = 64
Y, X, ZH, ZL, CORE = AXES = ("dp_0", "dp_1", "dp_2", "pipe_0", "pipe_1")
DP = AXES[:3]
PIPE = AXES[3:]
F32 = jnp.float32
BF16 = jnp.bfloat16

FIRST = (Y,)
FIRST_CAP = 24
SECOND = (ZH, X)
SECOND_CAP = 24
NORM_1 = (Y, X, CORE)
NORM_2 = (ZH, ZL)


def axis_size(axes):
    return math.prod({Y: 8, X: 4, ZH: 3, ZL: 4, CORE: 2}[a] for a in axes)


def floor_div(value, by):
    return jnp.floor((value + 0.5) * (1.0 / by))


def place(code, axes):
    y = floor_div(code - 1.0, 12 * VOC_DEV)
    rest = code - 1.0 - y * (12 * VOC_DEV)
    x = floor_div(rest, 3 * VOC_DEV)
    zh = floor_div(rest - x * (3 * VOC_DEV), VOC_DEV)
    index = 0.0
    for axis in axes:
        index = index * axis_size((axis,)) + {Y: y, X: x, ZH: zh}[axis]
    return index


def square_iota(n):
    return (lax.broadcasted_iota(jnp.int32, (n, n), 0), lax.broadcasted_iota(jnp.int32, (n, n), 1))


def column_to_row(column):
    i, j = square_iota(column.shape[0])
    return jnp.sum(jnp.where(i == j, column, 0.0), axis=0, keepdims=True)


def row_to_column(row):
    i, j = square_iota(row.shape[1])
    return jnp.sum(jnp.where(i == j, row, 0.0), axis=1, keepdims=True)


def decode(tail):
    lane = lax.broadcasted_iota(jnp.int32, (1, 128), 1)
    weight = jnp.where(lane == AUX, 1024.0, jnp.where(lane == AUX + 1, 8.0, jnp.where(lane == AUX + 2, 1.0, 0.0)))
    return jnp.sum(tail.astype(F32) * weight, axis=1, keepdims=True)


def encode(code):
    high = jnp.floor(code * (1.0 / 1024))
    rest = code - high * 1024.0
    middle = jnp.floor(rest * (1.0 / 8))
    low = rest - middle * 8.0
    lane = lax.broadcasted_iota(jnp.int32, (1, 128), 1)
    return jnp.where(lane == AUX, high, jnp.where(lane == AUX + 1, middle, jnp.where(lane == AUX + 2, low, 0.0)))


def pack(code_row, code_col, axes, cap):
    n = code_row.shape[1]
    i, j = square_iota(n)
    real_row = code_row > 0.5
    real_col = code_col > 0.5
    to_row = jnp.where(real_row, place(code_row, axes), -1.0)
    to_col = jnp.where(real_col, place(code_col, axes), -1.0)
    same = jnp.where((code_col == code_row) & real_row, 1.0, 0.0)
    above = jnp.where(i < j, same, 0.0)
    below = jnp.where(j < i, same, 0.0)
    count_row = jnp.sum(same, axis=0, keepdims=True)
    lead_row = (jnp.sum(above, axis=0, keepdims=True) == 0.0) & real_row
    lead_col = (jnp.sum(below, axis=1, keepdims=True) == 0.0) & real_col
    width_row = jnp.where(lead_row, jnp.minimum(count_row, 2.0), 0.0)
    before = jnp.sum(jnp.where((to_col == to_row) & (j < i), width_row, 0.0), axis=1, keepdims=True)
    before = jnp.where(lead_col, before, 0.0)
    slot_in = jnp.sum(same * before, axis=0, keepdims=True)
    over = jnp.max(jnp.where(real_row & (slot_in + jnp.minimum(count_row, 2.0) > cap), 1.0, 0.0), axis=1, keepdims=True)
    base = jnp.where(real_row, to_row * cap + slot_in, -2.0)
    return base, count_row, lead_row, over


def fill(out_ref, base, count_row, lead_row, code_row, head, tail, slots):
    n = base.shape[1]
    slot = lax.broadcasted_iota(jnp.int32, (slots, n), 0).astype(F32)
    first = slot == base
    second = (slot == base + 1.0) & (count_row > 1.5)
    take = jnp.where(first | second, 1.0, 0.0)
    code = jnp.sum(jnp.where(lead_row, take * code_row, 0.0), axis=1, keepdims=True)
    is_second = jnp.max(jnp.where(second, 1.0, 0.0), axis=1, keepdims=True) > 0.5
    take = take.astype(BF16)

    def split(rows):
        total = jnp.dot(take, rows, preferred_element_type=F32)
        kept = total.astype(BF16).astype(F32)
        return jnp.where(is_second, total - kept, kept)

    out_ref[:, :TAIL] = split(head).astype(BF16)
    lane = lax.broadcasted_iota(jnp.int32, (1, 128), 1)
    out_ref[:, TAIL:] = jnp.where(lane < AUX, split(tail), encode(code)).astype(BF16)


def first_kernel(grad_hbm, ids_ref, out_ref, over_ref, grad_ref, sem):
    load = pltpu.make_async_copy(grad_hbm, grad_ref, sem)
    load.start()
    code_row = ids_ref[...].astype(F32) + 1.0
    code_col = row_to_column(code_row)
    slots = out_ref.shape[0]
    base, count, lead, over = pack(code_row, code_col, FIRST, FIRST_CAP)
    over_ref[...] = jnp.broadcast_to(over, over_ref.shape)
    load.wait()
    tail = grad_ref[:, TAIL:]
    tail = jnp.concatenate([tail, jnp.zeros_like(tail)], axis=1)
    fill(out_ref, base, count, lead, code_row, grad_ref[:, :TAIL], tail, slots)


def second_kernel(rows_ref, over_in_ref, out_ref, over_ref):
    tail = rows_ref[:, TAIL:]
    code_col = decode(tail)
    code_row = column_to_row(code_col)
    base, count, lead, over = pack(code_row, code_col, SECOND, SECOND_CAP)
    fill(out_ref, base, count, lead, code_row, rows_ref[:, :TAIL], tail, out_ref.shape[0])
    over_ref[...] = jnp.broadcast_to(over, over_ref.shape) + over_in_ref[...]


def features(rows_ref):
    lane = lax.broadcasted_iota(jnp.int32, (1, 128), 1)
    tail = rows_ref[:, TAIL:]
    return rows_ref[:, :TAIL], jnp.where(lane < AUX, tail.astype(F32), 0.0).astype(BF16)


def norm_kernel(rows_ref, over_ref, part_ref):
    code_col = decode(rows_ref[:, TAIL:])
    code_row = column_to_row(code_col)
    head, tail = features(rows_ref)
    nt = (((1,), (1,)), ((), ()))
    gram = lax.dot_general(head, head, nt, preferred_element_type=F32)
    gram = gram + lax.dot_general(tail, tail, nt, preferred_element_type=F32)
    gram = jnp.where((code_col == code_row) & (code_row > 0.5), gram, 0.0)
    squares = jnp.sum(jnp.sum(gram, axis=0, keepdims=True), axis=1, keepdims=True)
    lane = lax.broadcasted_iota(jnp.int32, (1, 128), 1)
    part = jnp.where(lane == 0, squares, jnp.where(lane == 1, over_ref[:1, :], 0.0))
    part_ref[...] = jnp.broadcast_to(part[:, None, :], part_ref.shape)


def clip_factor(total, tokens):
    grad_norm = jnp.sqrt(total * float(D) + 1e-06)
    return jnp.minimum(1.0, 0.2 * math.sqrt(tokens * D) / grad_norm)


EDGES = (0, 384, 768, 1152, VOC_DEV)


def write_kernel(rows_ref, parts_ref, out_hbm, made_ref, sems, *, tokens):
    turned = rows_ref[...].T[: made_ref.shape[0], :]
    lane = lax.broadcasted_iota(jnp.int32, (1, 128), 1)
    total = jnp.sum(parts_ref[...], axis=0)
    total = jnp.sum(jnp.where(lane == 0, total, 0.0), axis=1, keepdims=True)
    scale = clip_factor(total, tokens) * math.sqrt(D)
    code = decode(rows_ref[:, TAIL:])
    local = code - 1.0
    local = jnp.where(code > 0.5, local - VOC_DEV * floor_div(local, VOC_DEV), -1.0).astype(jnp.int32)
    copies = []
    for k, (low, high) in enumerate(zip(EDGES[:-1], EDGES[1:])):
        here = lax.broadcasted_iota(jnp.int32, (local.shape[0], high - low), 1) + low
        pick = jnp.where(here == local, 1.0, 0.0).astype(BF16)
        made_ref[:, low:high] = jnp.dot(turned, pick, preferred_element_type=F32) * scale
        copies.append(pltpu.make_async_copy(made_ref.at[:, low:high], out_hbm.at[:, low:high], sems.at[k]))
        copies[-1].start()
    for copy in copies:
        copy.wait()


def shape(rows, cols, dtype=F32):
    return jax.ShapeDtypeStruct((rows, cols), dtype)


def near(dims, dtype=F32):
    return pltpu.VMEM(dims, dtype)


def around(axes, sizes, value, body, init):
    if not axes:
        return value, body(value, init)
    axis, n = axes[0], sizes[0]
    ring = [(k, (k + 1) % n) for k in range(n)]

    def step(_, carry):
        held, acc = around(axes[1:], sizes[1:], carry[0], body, carry[1])
        return jax.tree.map(lambda a: lax.ppermute(a, axis, ring), held), acc

    return lax.fori_loop(0, n, step, (value, init))


def general(embed_grad, ids):
    tokens = ids.shape[0]
    offset = lax.axis_index(DP) * VOC_DEV

    def add(held, acc):
        rows, names = held
        here = lax.broadcasted_iota(jnp.int32, (VOC_DEV, tokens), 0)
        pick = (here == (names[0] - offset)[None, :]).astype(BF16)
        return acc + jnp.dot(pick, rows, preferred_element_type=F32)

    names = jnp.broadcast_to(ids[None, :], (8, tokens))
    cols = embed_grad.shape[1]
    padded = jnp.pad(embed_grad, ((0, 0), (0, WIDE - cols)))
    _, summed = around(DP, (8, 4, 3), (padded, names), add, jnp.zeros((VOC_DEV, WIDE), F32))
    summed = summed[:, :cols]
    total = jnp.sum(summed * summed)
    for axis in AXES:
        total = lax.psum(total, axis)
    return summed * (clip_factor(total, tokens * 96) * math.sqrt(D))


def per_device(embed_grad, ids):
    tokens = ids.shape[0]
    cols = embed_grad.shape[1]
    slots_1 = axis_size(FIRST) * FIRST_CAP
    slots_2 = axis_size(SECOND) * SECOND_CAP
    sent, over = pl.pallas_call(
        first_kernel,
        in_specs=[pl.BlockSpec(memory_space=pltpu.HBM), pl.BlockSpec(memory_space=pltpu.VMEM)],
        out_shape=(near((slots_1, WIDE), BF16), near((8, 128))),
        scratch_shapes=[pltpu.VMEM((tokens, cols), BF16), pltpu.SemaphoreType.DMA],
        name="first",
    )(pltpu.with_memory_space_constraint(embed_grad, pltpu.HBM), ids.reshape(1, tokens))
    held = lax.all_to_all(sent, FIRST, 0, 0, tiled=True)
    sent, over = pl.pallas_call(second_kernel, out_shape=(near((slots_2, WIDE), BF16), near((8, 128))), name="second")(
        held, over
    )
    held = lax.all_to_all(sent, SECOND, 0, 0, tiled=True)
    n1, n2 = axis_size(NORM_1), axis_size(NORM_2)
    part = pl.pallas_call(norm_kernel, out_shape=near((n1, 1, 128)), name="squares")(held, over)
    part = lax.all_to_all(part, NORM_1, 0, 0, tiled=True)
    part = jnp.broadcast_to(jnp.sum(part, axis=0, keepdims=True), (n2, 1, 128))
    part = lax.all_to_all(part, NORM_2, 0, 0, tiled=True)
    overflow = jnp.sum(part[:, 0, 1])

    def routed():
        return pl.pallas_call(
            functools.partial(write_kernel, tokens=tokens * 96),
            in_specs=[pl.BlockSpec(memory_space=pltpu.VMEM)] * 2,
            out_specs=pl.BlockSpec(memory_space=pltpu.HBM),
            out_shape=shape(cols, VOC_DEV),
            scratch_shapes=[pltpu.VMEM((cols, VOC_DEV), F32), pltpu.SemaphoreType.DMA((len(EDGES) - 1,))],
            name="rows",
        )(held, part).T

    return lax.cond(overflow > 0.0, lambda: general(embed_grad, ids), routed)


def solution(mesh):
    torus = Mesh(mesh.devices.reshape(8, 4, 3, 4, 2), AXES)
    return jax.shard_map(
        per_device,
        mesh=torus,
        in_specs=(P(DP, PIPE), P(DP)),
        out_specs=P(DP, PIPE),
        check_vma=False,
    )
```

```python
import functools
import math

import jax
import jax.numpy as jnp
from jax import lax
from jax.experimental import pallas as pl
from jax.experimental.pallas import tpu as pltpu
from jax.sharding import Mesh
from jax.sharding import PartitionSpec as P

D = 4608
VOC_DEV = 1408
WIDE = 640
TAIL = 512
AUX = 64
Y, X, ZH, ZL, CORE = AXES = ("dp_0", "dp_1", "dp_2", "pipe_0", "pipe_1")
DP = AXES[:3]
PIPE = AXES[3:]
F32 = jnp.float32
BF16 = jnp.bfloat16

FIRST = (Y,)
FIRST_CAP = 24
SECOND = (ZH, X)
SECOND_CAP = 16
FAR = 4096.0
NORM_1 = (Y, X, CORE)
NORM_2 = (ZH, ZL)


def axis_size(axes):
    return math.prod({Y: 8, X: 4, ZH: 3, ZL: 4, CORE: 2}[a] for a in axes)


def floor_div(value, by):
    return jnp.floor((value + 0.5) * (1.0 / by))


def place(code, axes):
    y = floor_div(code - 1.0, 12 * VOC_DEV)
    rest = code - 1.0 - y * (12 * VOC_DEV)
    x = floor_div(rest, 3 * VOC_DEV)
    zh = floor_div(rest - x * (3 * VOC_DEV), VOC_DEV)
    index = 0.0
    for axis in axes:
        index = index * axis_size((axis,)) + {Y: y, X: x, ZH: zh}[axis]
    return index


def square_iota(n):
    return (lax.broadcasted_iota(jnp.int32, (n, n), 0), lax.broadcasted_iota(jnp.int32, (n, n), 1))


def column_to_row(column):
    i, j = square_iota(column.shape[0])
    return jnp.sum(jnp.where(i == j, column, 0.0), axis=0, keepdims=True)


def row_to_column(row):
    i, j = square_iota(row.shape[1])
    return jnp.sum(jnp.where(i == j, row, 0.0), axis=1, keepdims=True)


def decode(tail):
    lane = lax.broadcasted_iota(jnp.int32, (1, 128), 1)
    weight = jnp.where(lane == AUX, 1024.0, jnp.where(lane == AUX + 1, 8.0, jnp.where(lane == AUX + 2, 1.0, 0.0)))
    return jnp.sum(tail.astype(F32) * weight, axis=1, keepdims=True)


def encode(code):
    high = jnp.floor(code * (1.0 / 1024))
    rest = code - high * 1024.0
    middle = jnp.floor(rest * (1.0 / 8))
    low = rest - middle * 8.0
    lane = lax.broadcasted_iota(jnp.int32, (1, 128), 1)
    return jnp.where(lane == AUX, high, jnp.where(lane == AUX + 1, middle, jnp.where(lane == AUX + 2, low, 0.0)))


def pack(code_row, code_col, axes):
    n = code_row.shape[1]
    i, j = square_iota(n)
    real_row = code_row > 0.5
    real_col = code_col > 0.5
    to_row = jnp.where(real_row, place(code_row, axes), -1.0)
    to_col = jnp.where(real_col, place(code_col, axes), -1.0)
    same = jnp.where((code_col == code_row) & real_row, 1.0, 0.0)
    above = jnp.where(i < j, same, 0.0)
    below = jnp.where(j < i, same, 0.0)
    count_row = jnp.sum(same, axis=0, keepdims=True)
    lead_row = (jnp.sum(above, axis=0, keepdims=True) == 0.0) & real_row
    lead_col = (jnp.sum(below, axis=1, keepdims=True) == 0.0) & real_col
    width_row = jnp.where(lead_row, jnp.minimum(count_row, 2.0), 0.0)
    before = jnp.sum(jnp.where((to_col == to_row) & (j < i), width_row, 0.0), axis=1, keepdims=True)
    before = jnp.where(lead_col, before, 0.0)
    slot_in = jnp.sum(same * before, axis=0, keepdims=True)
    most = jnp.max(jnp.where(real_row, slot_in + jnp.minimum(count_row, 2.0), 0.0), axis=1, keepdims=True)
    return to_row, slot_in, count_row, lead_row, most


def fill(out_ref, where, cap, turn, code_row, head, tail):
    to_row, slot_in, count_row, lead_row, _ = where
    slots = out_ref.shape[0]
    slot = lax.broadcasted_iota(jnp.int32, (slots, to_row.shape[1]), 0).astype(F32)
    slot_in = slot_in - float(turn * cap)

    def at(place_in, valid):
        fits = valid & (to_row > -0.5) & (place_in > -0.5) & (place_in < cap - 0.5)
        return slot == jnp.where(fits, to_row * cap + place_in, -1.0)

    first = at(slot_in, True)
    second = at(slot_in + 1.0, count_row > 1.5)
    take = jnp.where(first | second, 1.0, 0.0)
    code = jnp.sum(jnp.where(lead_row, take * code_row, 0.0), axis=1, keepdims=True)
    is_second = jnp.max(jnp.where(second, 1.0, 0.0), axis=1, keepdims=True) > 0.5
    take = take.astype(BF16)

    def split(rows):
        total = jnp.dot(take, rows, preferred_element_type=F32)
        kept = total.astype(BF16).astype(F32)
        return jnp.where(is_second, total - kept, kept)

    out_ref[:, :TAIL] = split(head).astype(BF16)
    lane = lax.broadcasted_iota(jnp.int32, (1, 128), 1)
    out_ref[:, TAIL:] = jnp.where(lane < AUX, split(tail), encode(code)).astype(BF16)


def first_kernel(grad_hbm, ids_ref, out_ref, over_ref, grad_ref, sem):
    load = pltpu.make_async_copy(grad_hbm, grad_ref, sem)
    load.start()
    code_row = ids_ref[...].astype(F32) + 1.0
    code_col = row_to_column(code_row)
    where = pack(code_row, code_col, FIRST)
    over_ref[...] = jnp.broadcast_to(jnp.where(where[-1] > FIRST_CAP, FAR, 0.0), over_ref.shape)
    load.wait()
    tail = grad_ref[:, TAIL:]
    tail = jnp.concatenate([tail, jnp.zeros_like(tail)], axis=1)
    fill(out_ref, where, FIRST_CAP, 0, code_row, grad_ref[:, :TAIL], tail)


def second_kernel(rows_ref, over_in_ref, out_ref, over_ref, *, turn):
    tail = rows_ref[:, TAIL:]
    code_col = decode(tail)
    code_row = column_to_row(code_col)
    where = pack(code_row, code_col, SECOND)
    fill(out_ref, where, SECOND_CAP, turn, code_row, rows_ref[:, :TAIL], tail)
    more = where[-1]
    over = jnp.where(more > 2 * SECOND_CAP, FAR, jnp.where(more > SECOND_CAP, 1.0, 0.0))
    over_ref[...] = jnp.broadcast_to(over, over_ref.shape) + over_in_ref[...]


def features(rows_ref):
    lane = lax.broadcasted_iota(jnp.int32, (1, 128), 1)
    tail = rows_ref[:, TAIL:]
    return rows_ref[:, :TAIL], jnp.where(lane < AUX, tail.astype(F32), 0.0).astype(BF16)


def norm_kernel(rows_ref, over_ref, part_ref):
    code_col = decode(rows_ref[:, TAIL:])
    code_row = column_to_row(code_col)
    head, tail = features(rows_ref)
    nt = (((1,), (1,)), ((), ()))
    gram = lax.dot_general(head, head, nt, preferred_element_type=F32)
    gram = gram + lax.dot_general(tail, tail, nt, preferred_element_type=F32)
    gram = jnp.where((code_col == code_row) & (code_row > 0.5), gram, 0.0)
    squares = jnp.sum(jnp.sum(gram, axis=0, keepdims=True), axis=1, keepdims=True)
    lane = lax.broadcasted_iota(jnp.int32, (1, 128), 1)
    part = jnp.where(lane == 0, squares, jnp.where(lane == 1, over_ref[:1, :], 0.0))
    part_ref[...] = jnp.broadcast_to(part[:, None, :], part_ref.shape)


def clip_factor(total, tokens):
    grad_norm = jnp.sqrt(total * float(D) + 1e-06)
    return jnp.minimum(1.0, 0.2 * math.sqrt(tokens * D) / grad_norm)


def relay_kernel(parts_ref, out_ref):
    out_ref[...] = jnp.broadcast_to(jnp.sum(parts_ref[...], axis=0, keepdims=True), out_ref.shape)


EDGES = (0, 256, 512, 768, 1024, 1280, VOC_DEV)


def write_kernel(rows_ref, parts_ref, out_hbm, made_ref, sems, *, tokens):
    turned = rows_ref[...].T[: made_ref.shape[0], :]
    lane = lax.broadcasted_iota(jnp.int32, (1, 128), 1)
    total = jnp.sum(parts_ref[...], axis=0)
    total = jnp.sum(jnp.where(lane == 0, total, 0.0), axis=1, keepdims=True)
    scale = clip_factor(total, tokens) * math.sqrt(D)
    code = decode(rows_ref[:, TAIL:])
    local = code - 1.0
    local = jnp.where(code > 0.5, local - VOC_DEV * floor_div(local, VOC_DEV), -1.0).astype(jnp.int32)
    copies = []
    for k, (low, high) in enumerate(zip(EDGES[:-1], EDGES[1:])):
        here = lax.broadcasted_iota(jnp.int32, (local.shape[0], high - low), 1) + low
        pick = jnp.where(here == local, 1.0, 0.0).astype(BF16)
        made_ref[:, low:high] = jnp.dot(turned, pick, preferred_element_type=F32) * scale
        copies.append(pltpu.make_async_copy(made_ref.at[:, low:high], out_hbm.at[:, low:high], sems.at[k]))
        copies[-1].start()
    for copy in copies:
        copy.wait()


def shape(rows, cols, dtype=F32):
    return jax.ShapeDtypeStruct((rows, cols), dtype)


def near(dims, dtype=F32):
    return pltpu.VMEM(dims, dtype)


def around(axes, sizes, value, body, init):
    if not axes:
        return value, body(value, init)
    axis, n = axes[0], sizes[0]
    ring = [(k, (k + 1) % n) for k in range(n)]

    def step(_, carry):
        held, acc = around(axes[1:], sizes[1:], carry[0], body, carry[1])
        return jax.tree.map(lambda a: lax.ppermute(a, axis, ring), held), acc

    return lax.fori_loop(0, n, step, (value, init))


def general(embed_grad, ids):
    tokens = ids.shape[0]
    offset = lax.axis_index(DP) * VOC_DEV

    def add(held, acc):
        rows, names = held
        here = lax.broadcasted_iota(jnp.int32, (VOC_DEV, tokens), 0)
        pick = (here == (names[0] - offset)[None, :]).astype(BF16)
        return acc + jnp.dot(pick, rows, preferred_element_type=F32)

    names = jnp.broadcast_to(ids[None, :], (8, tokens))
    cols = embed_grad.shape[1]
    padded = jnp.pad(embed_grad, ((0, 0), (0, WIDE - cols)))
    _, summed = around(DP, (8, 4, 3), (padded, names), add, jnp.zeros((VOC_DEV, WIDE), F32))
    summed = summed[:, :cols]
    total = jnp.sum(summed * summed)
    for axis in AXES:
        total = lax.psum(total, axis)
    return summed * (clip_factor(total, tokens * 96) * math.sqrt(D))


def kernel(body, out_shape, name, **more):
    vmem = pl.BlockSpec(memory_space=pltpu.VMEM)

    def call(*arrays):
        held = [pltpu.with_memory_space_constraint(a, pltpu.VMEM) for a in arrays]
        return pl.pallas_call(body, in_specs=[vmem] * len(held), out_shape=out_shape, name=name, **more)(*held)

    return call


def send_on(held, over, turn):
    slots = axis_size(SECOND) * SECOND_CAP
    body = functools.partial(second_kernel, turn=turn)
    sent, over = kernel(body, (near((slots, WIDE), BF16), near((8, 128))), "second")(held, over)
    return lax.all_to_all(sent, SECOND, 0, 0, tiled=True), over


def norm_parts(rows, over):
    n1, n2 = axis_size(NORM_1), axis_size(NORM_2)
    part = kernel(norm_kernel, near((n1, 1, 128)), "squares")(rows, over)
    part = lax.all_to_all(part, NORM_1, 0, 0, tiled=True)
    part = kernel(relay_kernel, near((n2, 1, 128)), "relay")(part)
    return lax.all_to_all(part, NORM_2, 0, 0, tiled=True)


def per_device(embed_grad, ids):
    tokens = ids.shape[0]
    cols = embed_grad.shape[1]
    slots_1 = axis_size(FIRST) * FIRST_CAP
    sent, over = pl.pallas_call(
        first_kernel,
        in_specs=[pl.BlockSpec(memory_space=pltpu.HBM), pl.BlockSpec(memory_space=pltpu.VMEM)],
        out_shape=(near((slots_1, WIDE), BF16), near((8, 128))),
        scratch_shapes=[pltpu.VMEM((tokens, cols), BF16), pltpu.SemaphoreType.DMA],
        name="first",
    )(pltpu.with_memory_space_constraint(embed_grad, pltpu.HBM), ids.reshape(1, tokens))
    held = lax.all_to_all(sent, FIRST, 0, 0, tiled=True)
    rows, over_all = send_on(held, over, 0)
    parts = norm_parts(rows, over_all)

    def written(rows, parts):
        return kernel(
            functools.partial(write_kernel, tokens=tokens * 96),
            shape(cols, VOC_DEV),
            "rows",
            out_specs=pl.BlockSpec(memory_space=pltpu.HBM),
            scratch_shapes=[pltpu.VMEM((cols, VOC_DEV), F32), pltpu.SemaphoreType.DMA((len(EDGES) - 1,))],
        )(rows, parts).T

    def longer():
        def extra():
            more, over_more = send_on(held, over, 1)
            both = jnp.concatenate([rows, more], axis=0)
            return written(both, norm_parts(both, over_more))

        return lax.cond(jnp.sum(parts[:, 0, 1]) > FAR - 0.5, lambda: general(embed_grad, ids), extra)

    return lax.cond(jnp.any(parts[:, 0, 1] > 0.5), longer, lambda: written(rows, parts))


def solution(mesh):
    torus = Mesh(mesh.devices.reshape(8, 4, 3, 4, 2), AXES)
    return jax.shard_map(
        per_device,
        mesh=torus,
        in_specs=(P(DP, PIPE), P(DP)),
        out_specs=P(DP, PIPE),
        check_vma=False,
    )
```

```python
import functools
import math

import jax
import jax.numpy as jnp
from jax import lax
from jax.experimental import pallas as pl
from jax.experimental.pallas import tpu as pltpu
from jax.sharding import Mesh
from jax.sharding import PartitionSpec as P

D = 4608
VOC_DEV = 1408
WIDE = 640
TAIL = 512
AUX = 64
Y, X, ZH, ZL, CORE = AXES = ("dp_0", "dp_1", "dp_2", "pipe_0", "pipe_1")
DP = AXES[:3]
PIPE = AXES[3:]
F32 = jnp.float32
BF16 = jnp.bfloat16

FIRST = (Y,)
FIRST_CAP = 24
SECOND = (ZH, X)
SECOND_CAP = 16
FAR = 4096.0
NORM_1 = (Y, X, CORE)
NORM_2 = (ZH, ZL)


def axis_size(axes):
    return math.prod({Y: 8, X: 4, ZH: 3, ZL: 4, CORE: 2}[a] for a in axes)


def floor_div(value, by):
    return jnp.floor((value + 0.5) * (1.0 / by))


def place(code, axes):
    y = floor_div(code - 1.0, 12 * VOC_DEV)
    rest = code - 1.0 - y * (12 * VOC_DEV)
    x = floor_div(rest, 3 * VOC_DEV)
    zh = floor_div(rest - x * (3 * VOC_DEV), VOC_DEV)
    index = 0.0
    for axis in axes:
        index = index * axis_size((axis,)) + {Y: y, X: x, ZH: zh}[axis]
    return index


def square_iota(n):
    return (lax.broadcasted_iota(jnp.int32, (n, n), 0), lax.broadcasted_iota(jnp.int32, (n, n), 1))


def column_to_row(column):
    i, j = square_iota(column.shape[0])
    return jnp.sum(jnp.where(i == j, column, 0.0), axis=0, keepdims=True)


def row_to_column(row):
    i, j = square_iota(row.shape[1])
    return jnp.sum(jnp.where(i == j, row, 0.0), axis=1, keepdims=True)


def decode(tail):
    lane = lax.broadcasted_iota(jnp.int32, (1, 128), 1)
    weight = jnp.where(lane == AUX, 1024.0, jnp.where(lane == AUX + 1, 8.0, jnp.where(lane == AUX + 2, 1.0, 0.0)))
    return jnp.sum(tail.astype(F32) * weight, axis=1, keepdims=True)


def encode(code):
    high = jnp.floor(code * (1.0 / 1024))
    rest = code - high * 1024.0
    middle = jnp.floor(rest * (1.0 / 8))
    low = rest - middle * 8.0
    lane = lax.broadcasted_iota(jnp.int32, (1, 128), 1)
    return jnp.where(lane == AUX, high, jnp.where(lane == AUX + 1, middle, jnp.where(lane == AUX + 2, low, 0.0)))


def pack(code_row, code_col, axes):
    n = code_row.shape[1]
    i, j = square_iota(n)
    real_row = code_row > 0.5
    real_col = code_col > 0.5
    to_row = jnp.where(real_row, place(code_row, axes), -1.0)
    to_col = jnp.where(real_col, place(code_col, axes), -1.0)
    same = jnp.where((code_col == code_row) & real_row, 1.0, 0.0)
    above = jnp.where(i < j, same, 0.0)
    below = jnp.where(j < i, same, 0.0)
    count_row = jnp.sum(same, axis=0, keepdims=True)
    lead_row = (jnp.sum(above, axis=0, keepdims=True) == 0.0) & real_row
    lead_col = (jnp.sum(below, axis=1, keepdims=True) == 0.0) & real_col
    width_row = jnp.where(lead_row, jnp.minimum(count_row, 2.0), 0.0)
    before = jnp.sum(jnp.where((to_col == to_row) & (j < i), width_row, 0.0), axis=1, keepdims=True)
    before = jnp.where(lead_col, before, 0.0)
    slot_in = jnp.sum(same * before, axis=0, keepdims=True)
    most = jnp.max(jnp.where(real_row, slot_in + jnp.minimum(count_row, 2.0), 0.0), axis=1, keepdims=True)
    return to_row, slot_in, count_row, lead_row, most


def fill(out_ref, where, cap, turn, code_row, head, tail):
    to_row, slot_in, count_row, lead_row, _ = where
    slots = out_ref.shape[0]
    slot = lax.broadcasted_iota(jnp.int32, (slots, to_row.shape[1]), 0).astype(F32)
    slot_in = slot_in - float(turn * cap)

    def at(place_in, valid):
        fits = valid & (to_row > -0.5) & (place_in > -0.5) & (place_in < cap - 0.5)
        return slot == jnp.where(fits, to_row * cap + place_in, -1.0)

    first = at(slot_in, True)
    second = at(slot_in + 1.0, count_row > 1.5)
    take = jnp.where(first | second, 1.0, 0.0)
    code = jnp.sum(jnp.where(lead_row, take * code_row, 0.0), axis=1, keepdims=True)
    is_second = jnp.max(jnp.where(second, 1.0, 0.0), axis=1, keepdims=True) > 0.5
    take = take.astype(BF16)

    def split(rows):
        total = jnp.dot(take, rows, preferred_element_type=F32)
        kept = total.astype(BF16).astype(F32)
        return jnp.where(is_second, total - kept, kept)

    out_ref[:, :TAIL] = split(head).astype(BF16)
    lane = lax.broadcasted_iota(jnp.int32, (1, 128), 1)
    out_ref[:, TAIL:] = jnp.where(lane < AUX, split(tail), encode(code)).astype(BF16)


def first_kernel(grad_hbm, ids_hbm, out_ref, over_ref, grad_ref, ids_ref, sems):
    load_ids = pltpu.make_async_copy(ids_hbm, ids_ref, sems.at[0])
    load = pltpu.make_async_copy(grad_hbm, grad_ref, sems.at[1])
    load_ids.start()
    load.start()
    load_ids.wait()
    code_row = ids_ref[...].astype(F32) + 1.0
    code_col = row_to_column(code_row)
    where = pack(code_row, code_col, FIRST)
    over_ref[...] = jnp.broadcast_to(jnp.where(where[-1] > FIRST_CAP, FAR, 0.0), over_ref.shape)
    load.wait()
    tail = grad_ref[:, TAIL:]
    tail = jnp.concatenate([tail, jnp.zeros_like(tail)], axis=1)
    fill(out_ref, where, FIRST_CAP, 0, code_row, grad_ref[:, :TAIL], tail)


def second_kernel(rows_ref, over_in_ref, out_ref, over_ref, *, turn):
    tail = rows_ref[:, TAIL:]
    code_col = decode(tail)
    code_row = column_to_row(code_col)
    where = pack(code_row, code_col, SECOND)
    fill(out_ref, where, SECOND_CAP, turn, code_row, rows_ref[:, :TAIL], tail)
    more = where[-1]
    over = jnp.where(more > 2 * SECOND_CAP, FAR, jnp.where(more > SECOND_CAP, 1.0, 0.0))
    over_ref[...] = jnp.broadcast_to(over, over_ref.shape) + over_in_ref[...]


def features(rows_ref):
    lane = lax.broadcasted_iota(jnp.int32, (1, 128), 1)
    tail = rows_ref[:, TAIL:]
    return rows_ref[:, :TAIL], jnp.where(lane < AUX, tail.astype(F32), 0.0).astype(BF16)


def norm_kernel(rows_ref, over_ref, part_ref):
    code_col = decode(rows_ref[:, TAIL:])
    code_row = column_to_row(code_col)
    head, tail = features(rows_ref)
    nt = (((1,), (1,)), ((), ()))
    gram = lax.dot_general(head, head, nt, preferred_element_type=F32)
    gram = gram + lax.dot_general(tail, tail, nt, preferred_element_type=F32)
    gram = jnp.where((code_col == code_row) & (code_row > 0.5), gram, 0.0)
    squares = jnp.sum(jnp.sum(gram, axis=0, keepdims=True), axis=1, keepdims=True)
    lane = lax.broadcasted_iota(jnp.int32, (1, 128), 1)
    part = jnp.where(lane == 0, squares, jnp.where(lane == 1, over_ref[:1, :], 0.0))
    part_ref[...] = jnp.broadcast_to(part[:, None, :], part_ref.shape)


def clip_factor(total, tokens):
    grad_norm = jnp.sqrt(total * float(D) + 1e-06)
    return jnp.minimum(1.0, 0.2 * math.sqrt(tokens * D) / grad_norm)


def relay_kernel(parts_ref, out_ref):
    out_ref[...] = jnp.broadcast_to(jnp.sum(parts_ref[...], axis=0, keepdims=True), out_ref.shape)


EDGES = (0, 256, 512, 768, 1024, 1280, VOC_DEV)


def write_kernel(rows_ref, parts_ref, out_hbm, short_ref, made_ref, sems, *, tokens):
    turned = rows_ref[...].T[: made_ref.shape[0], :]
    lane = lax.broadcasted_iota(jnp.int32, (1, 128), 1)
    parts = jnp.sum(parts_ref[...], axis=0)
    total = jnp.sum(jnp.where(lane == 0, parts, 0.0), axis=1, keepdims=True)
    short_ref[0] = jnp.max(jnp.where(lane == 1, parts, 0.0)).astype(jnp.int32)
    scale = clip_factor(total, tokens) * math.sqrt(D)
    code = decode(rows_ref[:, TAIL:])
    local = code - 1.0
    local = jnp.where(code > 0.5, local - VOC_DEV * floor_div(local, VOC_DEV), -1.0).astype(jnp.int32)
    copies = []
    for k, (low, high) in enumerate(zip(EDGES[:-1], EDGES[1:])):
        here = lax.broadcasted_iota(jnp.int32, (local.shape[0], high - low), 1) + low
        pick = jnp.where(here == local, 1.0, 0.0).astype(BF16)
        made_ref[:, low:high] = jnp.dot(turned, pick, preferred_element_type=F32) * scale
        copies.append(pltpu.make_async_copy(made_ref.at[:, low:high], out_hbm.at[:, low:high], sems.at[k]))
        copies[-1].start()
    for copy in copies:
        copy.wait()


def shape(rows, cols, dtype=F32):
    return jax.ShapeDtypeStruct((rows, cols), dtype)


def near(dims, dtype=F32):
    return pltpu.VMEM(dims, dtype)


def times_kernel(sums_ref, scale_ref, out_ref):
    out_ref[...] = sums_ref[...] * scale_ref[...]


def around(axes, sizes, value, body, init):
    if not axes:
        return value, body(value, init)
    axis, n = axes[0], sizes[0]
    ring = [(k, (k + 1) % n) for k in range(n)]

    def step(_, carry):
        held, acc = around(axes[1:], sizes[1:], carry[0], body, carry[1])
        return jax.tree.map(lambda a: lax.ppermute(a, axis, ring), held), acc

    return lax.fori_loop(0, n, step, (value, init))


def general(embed_grad, ids):
    tokens = ids.shape[0]
    offset = lax.axis_index(DP) * VOC_DEV

    def add(held, acc):
        rows, names = held
        here = lax.broadcasted_iota(jnp.int32, (VOC_DEV, tokens), 0)
        pick = (here == (names[0] - offset)[None, :]).astype(BF16)
        return acc + jnp.dot(pick, rows, preferred_element_type=F32)

    names = jnp.broadcast_to(ids[None, :], (8, tokens))
    cols = embed_grad.shape[1]
    padded = jnp.pad(embed_grad, ((0, 0), (0, WIDE - cols)))
    _, summed = around(DP, (8, 4, 3), (padded, names), add, jnp.zeros((VOC_DEV, WIDE), F32))
    summed = summed[:, :cols]
    total = jnp.sum(summed * summed)
    for axis in AXES:
        total = lax.psum(total, axis)
    scale = clip_factor(total, tokens * 96) * math.sqrt(D)
    return pl.pallas_call(times_kernel, out_shape=shape(cols, VOC_DEV), name="times")(summed.T, scale.reshape(1, 1))


def kernel(body, out_shape, name, **more):
    vmem = pl.BlockSpec(memory_space=pltpu.VMEM)

    def call(*arrays):
        held = [pltpu.with_memory_space_constraint(a, pltpu.VMEM) for a in arrays]
        return pl.pallas_call(body, in_specs=[vmem] * len(held), out_shape=out_shape, name=name, **more)(*held)

    return call


def send_on(held, over, turn):
    slots = axis_size(SECOND) * SECOND_CAP
    body = functools.partial(second_kernel, turn=turn)
    sent, over = kernel(body, (near((slots, WIDE), BF16), near((8, 128))), "second")(held, over)
    return lax.all_to_all(sent, SECOND, 0, 0, tiled=True), over


def norm_parts(rows, over):
    n1, n2 = axis_size(NORM_1), axis_size(NORM_2)
    part = kernel(norm_kernel, near((n1, 1, 128)), "squares")(rows, over)
    part = lax.all_to_all(part, NORM_1, 0, 0, tiled=True)
    part = kernel(relay_kernel, near((n2, 1, 128)), "relay")(part)
    return lax.all_to_all(part, NORM_2, 0, 0, tiled=True)


def send_first(embed_grad, ids):
    tokens, cols = embed_grad.shape
    slots_1 = axis_size(FIRST) * FIRST_CAP
    hbm = pl.BlockSpec(memory_space=pltpu.HBM)
    sent, over = pl.pallas_call(
        first_kernel,
        in_specs=[hbm, hbm],
        out_shape=(near((slots_1, WIDE), BF16), near((8, 128))),
        scratch_shapes=[
            pltpu.VMEM((tokens, cols), BF16),
            pltpu.VMEM((1, tokens), jnp.int32),
            pltpu.SemaphoreType.DMA((2,)),
        ],
        name="first",
    )(*[pltpu.with_memory_space_constraint(a, pltpu.HBM) for a in (embed_grad, ids.reshape(1, tokens))])
    return lax.all_to_all(sent, FIRST, 0, 0, tiled=True), over


def per_device(embed_grad, ids):
    tokens, cols = embed_grad.shape

    def written(rows, parts):
        return kernel(
            functools.partial(write_kernel, tokens=tokens * 96),
            (shape(cols, VOC_DEV), jax.ShapeDtypeStruct((1,), jnp.int32)),
            "rows",
            out_specs=(pl.BlockSpec(memory_space=pltpu.HBM), pl.BlockSpec(memory_space=pltpu.SMEM)),
            scratch_shapes=[pltpu.VMEM((cols, VOC_DEV), F32), pltpu.SemaphoreType.DMA((len(EDGES) - 1,))],
        )(rows, parts)

    def again(state):
        def extra():
            held, over = send_first(embed_grad, ids)
            rows, over_all = send_on(held, over, 0)
            more, _ = send_on(held, over, 1)
            both = jnp.concatenate([rows, more], axis=0)
            return written(both, norm_parts(both, over_all))[0]

        out = lax.cond(state[1] >= int(FAR), lambda: general(embed_grad, ids), extra)
        return out, jnp.int32(0)

    held, over = send_first(embed_grad, ids)
    rows, over = send_on(held, over, 0)
    out, short = written(rows, norm_parts(rows, over))
    out, _ = lax.while_loop(lambda state: state[1] > 0, again, (out, short[0]))
    return out.T


def solution(mesh):
    torus = Mesh(mesh.devices.reshape(8, 4, 3, 4, 2), AXES)
    return jax.shard_map(
        per_device,
        mesh=torus,
        in_specs=(P(DP, PIPE), P(DP)),
        out_specs=P(DP, PIPE),
        check_vma=False,
    )
```

```python
import functools
import math

import jax
import jax.numpy as jnp
from jax import lax
from jax.experimental import pallas as pl
from jax.experimental.pallas import tpu as pltpu
from jax.sharding import Mesh
from jax.sharding import PartitionSpec as P

D = 4608
VOC_DEV = 1408
WIDE = 640
TAIL = 512
AUX = 64
Y, X, ZH, ZL, CORE = AXES = ("dp_0", "dp_1", "dp_2", "pipe_0", "pipe_1")
DP = AXES[:3]
PIPE = AXES[3:]
F32 = jnp.float32
BF16 = jnp.bfloat16

FIRST = (Y,)
FIRST_CAP = 24
SECOND = (X, ZH)
SECOND_CAP = 16
FAR = 4096.0
NORM_1 = (Y, X, CORE)
NORM_2 = (ZH, ZL)


def axis_size(axes):
    return math.prod({Y: 8, X: 4, ZH: 3, ZL: 4, CORE: 2}[a] for a in axes)


def floor_div(value, by):
    return jnp.floor((value + 0.5) * (1.0 / by))


def place(code, axes):
    y = floor_div(code - 1.0, 12 * VOC_DEV)
    rest = code - 1.0 - y * (12 * VOC_DEV)
    x = floor_div(rest, 3 * VOC_DEV)
    zh = floor_div(rest - x * (3 * VOC_DEV), VOC_DEV)
    index = 0.0
    for axis in axes:
        index = index * axis_size((axis,)) + {Y: y, X: x, ZH: zh}[axis]
    return index


def square_iota(n):
    return (lax.broadcasted_iota(jnp.int32, (n, n), 0), lax.broadcasted_iota(jnp.int32, (n, n), 1))


def column_to_row(column):
    i, j = square_iota(column.shape[0])
    return jnp.sum(jnp.where(i == j, column, 0.0), axis=0, keepdims=True)


def row_to_column(row):
    i, j = square_iota(row.shape[1])
    return jnp.sum(jnp.where(i == j, row, 0.0), axis=1, keepdims=True)


def decode(tail):
    lane = lax.broadcasted_iota(jnp.int32, (1, 128), 1)
    weight = jnp.where(lane == AUX, 1024.0, jnp.where(lane == AUX + 1, 8.0, jnp.where(lane == AUX + 2, 1.0, 0.0)))
    return jnp.sum(tail.astype(F32) * weight, axis=1, keepdims=True)


def encode(code):
    high = jnp.floor(code * (1.0 / 1024))
    rest = code - high * 1024.0
    middle = jnp.floor(rest * (1.0 / 8))
    low = rest - middle * 8.0
    lane = lax.broadcasted_iota(jnp.int32, (1, 128), 1)
    return jnp.where(lane == AUX, high, jnp.where(lane == AUX + 1, middle, jnp.where(lane == AUX + 2, low, 0.0)))


def pack(code_row, code_col, axes):
    n = code_row.shape[1]
    i, j = square_iota(n)
    real_row = code_row > 0.5
    real_col = code_col > 0.5
    to_row = jnp.where(real_row, place(code_row, axes), -1.0)
    to_col = jnp.where(real_col, place(code_col, axes), -1.0)
    same = jnp.where((code_col == code_row) & real_row, 1.0, 0.0)
    above = jnp.where(i < j, same, 0.0)
    below = jnp.where(j < i, same, 0.0)
    count_row = jnp.sum(same, axis=0, keepdims=True)
    lead_row = (jnp.sum(above, axis=0, keepdims=True) == 0.0) & real_row
    lead_col = (jnp.sum(below, axis=1, keepdims=True) == 0.0) & real_col
    width_row = jnp.where(lead_row, jnp.minimum(count_row, 2.0), 0.0)
    before = jnp.sum(jnp.where((to_col == to_row) & (j < i), width_row, 0.0), axis=1, keepdims=True)
    before = jnp.where(lead_col, before, 0.0)
    slot_in = jnp.sum(same * before, axis=0, keepdims=True)
    most = jnp.max(jnp.where(real_row, slot_in + jnp.minimum(count_row, 2.0), 0.0), axis=1, keepdims=True)
    return to_row, slot_in, count_row, lead_row, most


def fill(out_ref, where, cap, turn, code_row, head, tail):
    to_row, slot_in, count_row, lead_row, _ = where
    slots = out_ref.shape[0]
    slot = lax.broadcasted_iota(jnp.int32, (slots, to_row.shape[1]), 0).astype(F32)
    slot_in = slot_in - float(turn * cap)

    def at(place_in, valid):
        fits = valid & (to_row > -0.5) & (place_in > -0.5) & (place_in < cap - 0.5)
        return slot == jnp.where(fits, to_row * cap + place_in, -1.0)

    first = at(slot_in, True)
    second = at(slot_in + 1.0, count_row > 1.5)
    take = jnp.where(first | second, 1.0, 0.0)
    code = jnp.sum(jnp.where(lead_row, take * code_row, 0.0), axis=1, keepdims=True)
    is_second = jnp.max(jnp.where(second, 1.0, 0.0), axis=1, keepdims=True) > 0.5
    take = take.astype(BF16)

    def split(rows):
        total = jnp.dot(take, rows, preferred_element_type=F32)
        kept = total.astype(BF16).astype(F32)
        return jnp.where(is_second, total - kept, kept)

    out_ref[:, :TAIL] = split(head).astype(BF16)
    lane = lax.broadcasted_iota(jnp.int32, (1, 128), 1)
    out_ref[:, TAIL:] = jnp.where(lane < AUX, split(tail), encode(code)).astype(BF16)


def first_kernel(grad_hbm, ids_hbm, out_ref, over_ref, grad_ref, ids_ref, sems):
    load_ids = pltpu.make_async_copy(ids_hbm, ids_ref, sems.at[0])
    load = pltpu.make_async_copy(grad_hbm, grad_ref, sems.at[1])
    load_ids.start()
    load.start()
    load_ids.wait()
    code_row = ids_ref[...].astype(F32) + 1.0
    code_col = row_to_column(code_row)
    where = pack(code_row, code_col, FIRST)
    over_ref[...] = jnp.broadcast_to(jnp.where(where[-1] > FIRST_CAP, FAR, 0.0), over_ref.shape)
    load.wait()
    tail = grad_ref[:, TAIL:]
    tail = jnp.concatenate([tail, jnp.zeros_like(tail)], axis=1)
    fill(out_ref, where, FIRST_CAP, 0, code_row, grad_ref[:, :TAIL], tail)


def second_kernel(rows_ref, over_in_ref, out_ref, over_ref, *, turn):
    tail = rows_ref[:, TAIL:]
    code_col = decode(tail)
    code_row = column_to_row(code_col)
    where = pack(code_row, code_col, SECOND)
    fill(out_ref, where, SECOND_CAP, turn, code_row, rows_ref[:, :TAIL], tail)
    more = where[-1]
    over = jnp.where(more > 2 * SECOND_CAP, FAR, jnp.where(more > SECOND_CAP, 1.0, 0.0))
    over_ref[...] = jnp.broadcast_to(over, over_ref.shape) + over_in_ref[...]


def features(rows_ref):
    lane = lax.broadcasted_iota(jnp.int32, (1, 128), 1)
    tail = rows_ref[:, TAIL:]
    return rows_ref[:, :TAIL], jnp.where(lane < AUX, tail.astype(F32), 0.0).astype(BF16)


def norm_kernel(rows_ref, over_ref, part_ref):
    code_col = decode(rows_ref[:, TAIL:])
    code_row = column_to_row(code_col)
    head, tail = features(rows_ref)
    nt = (((1,), (1,)), ((), ()))
    gram = lax.dot_general(head, head, nt, preferred_element_type=F32)
    gram = gram + lax.dot_general(tail, tail, nt, preferred_element_type=F32)
    gram = jnp.where((code_col == code_row) & (code_row > 0.5), gram, 0.0)
    squares = jnp.sum(jnp.sum(gram, axis=0, keepdims=True), axis=1, keepdims=True)
    lane = lax.broadcasted_iota(jnp.int32, (1, 128), 1)
    part = jnp.where(lane == 0, squares, jnp.where(lane == 1, over_ref[:1, :], 0.0))
    part_ref[...] = jnp.broadcast_to(part[:, None, :], part_ref.shape)


def clip_factor(total, tokens):
    grad_norm = jnp.sqrt(total * float(D) + 1e-06)
    return jnp.minimum(1.0, 0.2 * math.sqrt(tokens * D) / grad_norm)


def relay_kernel(parts_ref, out_ref):
    out_ref[...] = jnp.broadcast_to(jnp.sum(parts_ref[...], axis=0, keepdims=True), out_ref.shape)


EDGES = (0, 256, 512, 768, 1024, 1280, VOC_DEV)


def write_kernel(rows_ref, parts_ref, out_hbm, short_hbm, made_ref, short_ref, sems, *, tokens):
    turned = rows_ref[...].T[: made_ref.shape[0], :]
    lane = lax.broadcasted_iota(jnp.int32, (1, 128), 1)
    parts = jnp.sum(parts_ref[...], axis=0)
    total = jnp.sum(jnp.where(lane == 0, parts, 0.0), axis=1, keepdims=True)
    short_ref[0] = jnp.max(jnp.where(lane == 1, parts, 0.0)).astype(jnp.int32)
    copies = [pltpu.make_async_copy(short_ref, short_hbm, sems.at[len(EDGES) - 1])]
    copies[0].start()
    scale = clip_factor(total, tokens) * math.sqrt(D)
    code = decode(rows_ref[:, TAIL:])
    local = code - 1.0
    local = jnp.where(code > 0.5, local - VOC_DEV * floor_div(local, VOC_DEV), -1.0).astype(jnp.int32)
    for k, (low, high) in enumerate(zip(EDGES[:-1], EDGES[1:])):
        here = lax.broadcasted_iota(jnp.int32, (local.shape[0], high - low), 1) + low
        pick = jnp.where(here == local, 1.0, 0.0).astype(BF16)
        made_ref[:, low:high] = jnp.dot(turned, pick, preferred_element_type=F32) * scale
        copies.append(pltpu.make_async_copy(made_ref.at[:, low:high], out_hbm.at[:, low:high], sems.at[k]))
        copies[-1].start()
    for copy in copies:
        copy.wait()


def shape(rows, cols, dtype=F32):
    return jax.ShapeDtypeStruct((rows, cols), dtype)


def near(dims, dtype=F32):
    return pltpu.VMEM(dims, dtype)


def times_kernel(sums_ref, scale_ref, out_ref):
    out_ref[...] = sums_ref[...] * scale_ref[...]


def around(axes, sizes, value, body, init):
    if not axes:
        return value, body(value, init)
    axis, n = axes[0], sizes[0]
    ring = [(k, (k + 1) % n) for k in range(n)]

    def step(_, carry):
        held, acc = around(axes[1:], sizes[1:], carry[0], body, carry[1])
        return jax.tree.map(lambda a: lax.ppermute(a, axis, ring), held), acc

    return lax.fori_loop(0, n, step, (value, init))


def general(embed_grad, ids):
    tokens = ids.shape[0]
    offset = lax.axis_index(DP) * VOC_DEV

    def add(held, acc):
        rows, names = held
        here = lax.broadcasted_iota(jnp.int32, (VOC_DEV, tokens), 0)
        pick = (here == (names[0] - offset)[None, :]).astype(BF16)
        return acc + jnp.dot(pick, rows, preferred_element_type=F32)

    names = jnp.broadcast_to(ids[None, :], (8, tokens))
    cols = embed_grad.shape[1]
    padded = jnp.pad(embed_grad, ((0, 0), (0, WIDE - cols)))
    _, summed = around(DP, (8, 4, 3), (padded, names), add, jnp.zeros((VOC_DEV, WIDE), F32))
    summed = summed[:, :cols]
    total = jnp.sum(summed * summed)
    for axis in AXES:
        total = lax.psum(total, axis)
    scale = clip_factor(total, tokens * 96) * math.sqrt(D)
    return pl.pallas_call(times_kernel, out_shape=shape(cols, VOC_DEV), name="times")(summed.T, scale.reshape(1, 1))


def kernel(body, out_shape, name, **more):
    vmem = pl.BlockSpec(memory_space=pltpu.VMEM)

    def call(*arrays):
        held = [pltpu.with_memory_space_constraint(a, pltpu.VMEM) for a in arrays]
        return pl.pallas_call(body, in_specs=[vmem] * len(held), out_shape=out_shape, name=name, **more)(*held)

    return call


def send_on(held, over, turn):
    slots = axis_size(SECOND) * SECOND_CAP
    body = functools.partial(second_kernel, turn=turn)
    sent, over = kernel(body, (near((slots, WIDE), BF16), near((8, 128))), "second")(held, over)
    return lax.all_to_all(sent, SECOND, 0, 0, tiled=True), over


def norm_parts(rows, over):
    n1, n2 = axis_size(NORM_1), axis_size(NORM_2)
    part = kernel(norm_kernel, near((n1, 1, 128)), "squares")(rows, over)
    part = lax.all_to_all(part, NORM_1, 0, 0, tiled=True)
    part = kernel(relay_kernel, near((n2, 1, 128)), "relay")(part)
    return lax.all_to_all(part, NORM_2, 0, 0, tiled=True)


def send_first(embed_grad, ids):
    tokens, cols = embed_grad.shape
    slots_1 = axis_size(FIRST) * FIRST_CAP
    hbm = pl.BlockSpec(memory_space=pltpu.HBM)
    sent, over = pl.pallas_call(
        first_kernel,
        in_specs=[hbm, hbm],
        out_shape=(near((slots_1, WIDE), BF16), near((8, 128))),
        scratch_shapes=[
            pltpu.VMEM((tokens, cols), BF16),
            pltpu.VMEM((1, tokens), jnp.int32),
            pltpu.SemaphoreType.DMA((2,)),
        ],
        name="first",
    )(*[pltpu.with_memory_space_constraint(a, pltpu.HBM) for a in (embed_grad, ids.reshape(1, tokens))])
    return lax.all_to_all(sent, FIRST, 0, 0, tiled=True), over


def per_device(embed_grad, ids):
    tokens, cols = embed_grad.shape

    def written(rows, parts):
        return kernel(
            functools.partial(write_kernel, tokens=tokens * 96),
            (shape(cols, VOC_DEV), jax.ShapeDtypeStruct((1,), jnp.int32)),
            "rows",
            out_specs=(pl.BlockSpec(memory_space=pltpu.HBM),) * 2,
            scratch_shapes=[
                pltpu.VMEM((cols, VOC_DEV), F32),
                pltpu.SMEM((1,), jnp.int32),
                pltpu.SemaphoreType.DMA((len(EDGES),)),
            ],
        )(rows, parts)

    def again(state):
        def extra():
            held, over = send_first(embed_grad, ids)
            rows, over_all = send_on(held, over, 0)
            more, _ = send_on(held, over, 1)
            both = jnp.concatenate([rows, more], axis=0)
            return written(both, norm_parts(both, over_all))[0]

        out = lax.cond(state[1] >= int(FAR), lambda: general(embed_grad, ids), extra)
        return out, jnp.int32(0)

    held, over = send_first(embed_grad, ids)
    rows, over = send_on(held, over, 0)
    out, short = written(rows, norm_parts(rows, over))
    out, _ = lax.while_loop(lambda state: state[1] > 0, again, (out, short[0]))
    return out.T


def solution(mesh):
    torus = Mesh(mesh.devices.reshape(8, 4, 3, 4, 2), AXES)
    return jax.shard_map(
        per_device,
        mesh=torus,
        in_specs=(P(DP, PIPE), P(DP)),
        out_specs=P(DP, PIPE),
        check_vma=False,
    )
```

```python
import functools
import math

import jax
import jax.numpy as jnp
from jax import lax
from jax.experimental import pallas as pl
from jax.experimental.pallas import tpu as pltpu
from jax.sharding import Mesh
from jax.sharding import PartitionSpec as P

D = 4608
VOC_DEV = 1408
WIDE = 640
TAIL = 512
AUX = 64
Y, X, ZH, ZL, CORE = AXES = ("dp_0", "dp_1", "dp_2", "pipe_0", "pipe_1")
DP = AXES[:3]
PIPE = AXES[3:]
F32 = jnp.float32
BF16 = jnp.bfloat16

FIRST = (Y,)
FIRST_CAP = 24
SECOND = (X, ZH)
SECOND_CAP = 16
FAR = 4096.0
NORM_1 = (ZH, ZL)
NORM_2 = (Y, X, CORE)


def axis_size(axes):
    return math.prod({Y: 8, X: 4, ZH: 3, ZL: 4, CORE: 2}[a] for a in axes)


def floor_div(value, by):
    return jnp.floor((value + 0.5) * (1.0 / by))


def place(code, axes):
    y = floor_div(code - 1.0, 12 * VOC_DEV)
    rest = code - 1.0 - y * (12 * VOC_DEV)
    x = floor_div(rest, 3 * VOC_DEV)
    zh = floor_div(rest - x * (3 * VOC_DEV), VOC_DEV)
    index = 0.0
    for axis in axes:
        index = index * axis_size((axis,)) + {Y: y, X: x, ZH: zh}[axis]
    return index


def square_iota(n):
    return (lax.broadcasted_iota(jnp.int32, (n, n), 0), lax.broadcasted_iota(jnp.int32, (n, n), 1))


def column_to_row(column):
    i, j = square_iota(column.shape[0])
    return jnp.sum(jnp.where(i == j, column, 0.0), axis=0, keepdims=True)


def row_to_column(row):
    i, j = square_iota(row.shape[1])
    return jnp.sum(jnp.where(i == j, row, 0.0), axis=1, keepdims=True)


def decode(tail):
    lane = lax.broadcasted_iota(jnp.int32, (1, 128), 1)
    weight = jnp.where(lane == AUX, 1024.0, jnp.where(lane == AUX + 1, 8.0, jnp.where(lane == AUX + 2, 1.0, 0.0)))
    return jnp.sum(tail.astype(F32) * weight, axis=1, keepdims=True)


def encode(code):
    high = jnp.floor(code * (1.0 / 1024))
    rest = code - high * 1024.0
    middle = jnp.floor(rest * (1.0 / 8))
    low = rest - middle * 8.0
    lane = lax.broadcasted_iota(jnp.int32, (1, 128), 1)
    return jnp.where(lane == AUX, high, jnp.where(lane == AUX + 1, middle, jnp.where(lane == AUX + 2, low, 0.0)))


def pack(code_row, code_col, axes):
    n = code_row.shape[1]
    i, j = square_iota(n)
    real_row = code_row > 0.5
    real_col = code_col > 0.5
    to_row = jnp.where(real_row, place(code_row, axes), -1.0)
    to_col = jnp.where(real_col, place(code_col, axes), -1.0)
    same = jnp.where((code_col == code_row) & real_row, 1.0, 0.0)
    above = jnp.where(i < j, same, 0.0)
    below = jnp.where(j < i, same, 0.0)
    count_row = jnp.sum(same, axis=0, keepdims=True)
    lead_row = (jnp.sum(above, axis=0, keepdims=True) == 0.0) & real_row
    lead_col = (jnp.sum(below, axis=1, keepdims=True) == 0.0) & real_col
    width_row = jnp.where(lead_row, jnp.minimum(count_row, 2.0), 0.0)
    before = jnp.sum(jnp.where((to_col == to_row) & (j < i), width_row, 0.0), axis=1, keepdims=True)
    before = jnp.where(lead_col, before, 0.0)
    slot_in = jnp.sum(same * before, axis=0, keepdims=True)
    most = jnp.max(jnp.where(real_row, slot_in + jnp.minimum(count_row, 2.0), 0.0), axis=1, keepdims=True)
    return to_row, slot_in, count_row, lead_row, most


def fill(out_ref, where, cap, turn, code_row, head, tail):
    to_row, slot_in, count_row, lead_row, _ = where
    slots = out_ref.shape[0]
    slot = lax.broadcasted_iota(jnp.int32, (slots, to_row.shape[1]), 0).astype(F32)
    slot_in = slot_in - float(turn * cap)

    def at(place_in, valid):
        fits = valid & (to_row > -0.5) & (place_in > -0.5) & (place_in < cap - 0.5)
        return slot == jnp.where(fits, to_row * cap + place_in, -1.0)

    first = at(slot_in, True)
    second = at(slot_in + 1.0, count_row > 1.5)
    take = jnp.where(first | second, 1.0, 0.0)
    code = jnp.sum(jnp.where(lead_row, take * code_row, 0.0), axis=1, keepdims=True)
    is_second = jnp.max(jnp.where(second, 1.0, 0.0), axis=1, keepdims=True) > 0.5
    take = take.astype(BF16)

    def split(rows):
        total = jnp.dot(take, rows, preferred_element_type=F32)
        kept = total.astype(BF16).astype(F32)
        return jnp.where(is_second, total - kept, kept)

    out_ref[:, :TAIL] = split(head).astype(BF16)
    lane = lax.broadcasted_iota(jnp.int32, (1, 128), 1)
    out_ref[:, TAIL:] = jnp.where(lane < AUX, split(tail), encode(code)).astype(BF16)


def first_kernel(grad_hbm, ids_hbm, out_ref, over_ref, grad_ref, ids_ref, sems):
    load_ids = pltpu.make_async_copy(ids_hbm, ids_ref, sems.at[0])
    load = pltpu.make_async_copy(grad_hbm, grad_ref, sems.at[1])
    load_ids.start()
    load.start()
    load_ids.wait()
    code_row = ids_ref[...].astype(F32) + 1.0
    code_col = row_to_column(code_row)
    where = pack(code_row, code_col, FIRST)
    over_ref[...] = jnp.broadcast_to(jnp.where(where[-1] > FIRST_CAP, FAR, 0.0), over_ref.shape)
    load.wait()
    tail = grad_ref[:, TAIL:]
    tail = jnp.concatenate([tail, jnp.zeros_like(tail)], axis=1)
    fill(out_ref, where, FIRST_CAP, 0, code_row, grad_ref[:, :TAIL], tail)


def second_kernel(rows_ref, over_in_ref, out_ref, over_ref, *, turn):
    tail = rows_ref[:, TAIL:]
    code_col = decode(tail)
    code_row = column_to_row(code_col)
    where = pack(code_row, code_col, SECOND)
    fill(out_ref, where, SECOND_CAP, turn, code_row, rows_ref[:, :TAIL], tail)
    more = where[-1]
    over = jnp.where(more > 2 * SECOND_CAP, FAR, jnp.where(more > SECOND_CAP, 1.0, 0.0))
    over_ref[...] = jnp.broadcast_to(over, over_ref.shape) + over_in_ref[...]


def features(rows_ref):
    lane = lax.broadcasted_iota(jnp.int32, (1, 128), 1)
    tail = rows_ref[:, TAIL:]
    return rows_ref[:, :TAIL], jnp.where(lane < AUX, tail.astype(F32), 0.0).astype(BF16)


def norm_kernel(rows_ref, over_ref, part_ref):
    code_col = decode(rows_ref[:, TAIL:])
    code_row = column_to_row(code_col)
    head, tail = features(rows_ref)
    nt = (((1,), (1,)), ((), ()))
    gram = lax.dot_general(head, head, nt, preferred_element_type=F32)
    gram = gram + lax.dot_general(tail, tail, nt, preferred_element_type=F32)
    gram = jnp.where((code_col == code_row) & (code_row > 0.5), gram, 0.0)
    squares = jnp.sum(jnp.sum(gram, axis=0, keepdims=True), axis=1, keepdims=True)
    lane = lax.broadcasted_iota(jnp.int32, (1, 128), 1)
    part = jnp.where(lane == 0, squares, jnp.where(lane == 1, over_ref[:1, :], 0.0))
    part_ref[...] = jnp.broadcast_to(part[:, None, :], part_ref.shape)


def clip_factor(total, tokens):
    grad_norm = jnp.sqrt(total * float(D) + 1e-06)
    return jnp.minimum(1.0, 0.2 * math.sqrt(tokens * D) / grad_norm)


def relay_kernel(parts_ref, out_ref):
    out_ref[...] = jnp.broadcast_to(jnp.sum(parts_ref[...], axis=0, keepdims=True), out_ref.shape)


EDGES = (0, 256, 512, 768, 1024, 1280, VOC_DEV)


def write_kernel(rows_ref, parts_ref, out_hbm, short_hbm, made_ref, short_ref, sems, *, tokens):
    turned = rows_ref[...].T[: made_ref.shape[0], :]
    lane = lax.broadcasted_iota(jnp.int32, (1, 128), 1)
    parts = jnp.sum(parts_ref[...], axis=0)
    total = jnp.sum(jnp.where(lane == 0, parts, 0.0), axis=1, keepdims=True)
    short_ref[0] = jnp.max(jnp.where(lane == 1, parts, 0.0)).astype(jnp.int32)
    copies = [pltpu.make_async_copy(short_ref, short_hbm, sems.at[len(EDGES) - 1])]
    copies[0].start()
    scale = clip_factor(total, tokens) * math.sqrt(D)
    code = decode(rows_ref[:, TAIL:])
    local = code - 1.0
    local = jnp.where(code > 0.5, local - VOC_DEV * floor_div(local, VOC_DEV), -1.0).astype(jnp.int32)
    for k, (low, high) in enumerate(zip(EDGES[:-1], EDGES[1:])):
        here = lax.broadcasted_iota(jnp.int32, (local.shape[0], high - low), 1) + low
        pick = jnp.where(here == local, 1.0, 0.0).astype(BF16)
        made_ref[:, low:high] = jnp.dot(turned, pick, preferred_element_type=F32) * scale
        copies.append(pltpu.make_async_copy(made_ref.at[:, low:high], out_hbm.at[:, low:high], sems.at[k]))
        copies[-1].start()
    for copy in copies:
        copy.wait()


def shape(rows, cols, dtype=F32):
    return jax.ShapeDtypeStruct((rows, cols), dtype)


def near(dims, dtype=F32):
    return pltpu.VMEM(dims, dtype)


def times_kernel(sums_ref, scale_ref, out_ref):
    out_ref[...] = sums_ref[...] * scale_ref[...]


def around(axes, sizes, value, body, init):
    if not axes:
        return value, body(value, init)
    axis, n = axes[0], sizes[0]
    ring = [(k, (k + 1) % n) for k in range(n)]

    def step(_, carry):
        held, acc = around(axes[1:], sizes[1:], carry[0], body, carry[1])
        return jax.tree.map(lambda a: lax.ppermute(a, axis, ring), held), acc

    return lax.fori_loop(0, n, step, (value, init))


def general(embed_grad, ids):
    tokens = ids.shape[0]
    offset = lax.axis_index(DP) * VOC_DEV

    def add(held, acc):
        rows, names = held
        here = lax.broadcasted_iota(jnp.int32, (VOC_DEV, tokens), 0)
        pick = (here == (names[0] - offset)[None, :]).astype(BF16)
        return acc + jnp.dot(pick, rows, preferred_element_type=F32)

    names = jnp.broadcast_to(ids[None, :], (8, tokens))
    cols = embed_grad.shape[1]
    padded = jnp.pad(embed_grad, ((0, 0), (0, WIDE - cols)))
    _, summed = around(DP, (8, 4, 3), (padded, names), add, jnp.zeros((VOC_DEV, WIDE), F32))
    summed = summed[:, :cols]
    total = jnp.sum(summed * summed)
    for axis in AXES:
        total = lax.psum(total, axis)
    scale = clip_factor(total, tokens * 96) * math.sqrt(D)
    return pl.pallas_call(times_kernel, out_shape=shape(cols, VOC_DEV), name="times")(summed.T, scale.reshape(1, 1))


def kernel(body, out_shape, name, **more):
    vmem = pl.BlockSpec(memory_space=pltpu.VMEM)

    def call(*arrays):
        held = [pltpu.with_memory_space_constraint(a, pltpu.VMEM) for a in arrays]
        return pl.pallas_call(body, in_specs=[vmem] * len(held), out_shape=out_shape, name=name, **more)(*held)

    return call


def send_on(held, over, turn):
    slots = axis_size(SECOND) * SECOND_CAP
    body = functools.partial(second_kernel, turn=turn)
    sent, over = kernel(body, (near((slots, WIDE), BF16), near((8, 128))), "second")(held, over)
    return lax.all_to_all(sent, SECOND, 0, 0, tiled=True), over


def norm_parts(rows, over):
    n1, n2 = axis_size(NORM_1), axis_size(NORM_2)
    part = kernel(norm_kernel, near((n1, 1, 128)), "squares")(rows, over)
    part = lax.all_to_all(part, NORM_1, 0, 0, tiled=True)
    part = kernel(relay_kernel, near((n2, 1, 128)), "relay")(part)
    return lax.all_to_all(part, NORM_2, 0, 0, tiled=True)


def send_first(embed_grad, ids):
    tokens, cols = embed_grad.shape
    slots_1 = axis_size(FIRST) * FIRST_CAP
    hbm = pl.BlockSpec(memory_space=pltpu.HBM)
    sent, over = pl.pallas_call(
        first_kernel,
        in_specs=[hbm, hbm],
        out_shape=(near((slots_1, WIDE), BF16), near((8, 128))),
        scratch_shapes=[
            pltpu.VMEM((tokens, cols), BF16),
            pltpu.VMEM((1, tokens), jnp.int32),
            pltpu.SemaphoreType.DMA((2,)),
        ],
        name="first",
    )(*[pltpu.with_memory_space_constraint(a, pltpu.HBM) for a in (embed_grad, ids.reshape(1, tokens))])
    return lax.all_to_all(sent, FIRST, 0, 0, tiled=True), over


def per_device(embed_grad, ids):
    tokens, cols = embed_grad.shape

    def written(rows, parts):
        return kernel(
            functools.partial(write_kernel, tokens=tokens * 96),
            (shape(cols, VOC_DEV), jax.ShapeDtypeStruct((1,), jnp.int32)),
            "rows",
            out_specs=(pl.BlockSpec(memory_space=pltpu.HBM),) * 2,
            scratch_shapes=[
                pltpu.VMEM((cols, VOC_DEV), F32),
                pltpu.SMEM((1,), jnp.int32),
                pltpu.SemaphoreType.DMA((len(EDGES),)),
            ],
        )(rows, parts)

    def again(state):
        def extra():
            held, over = send_first(embed_grad, ids)
            rows, over_all = send_on(held, over, 0)
            more, _ = send_on(held, over, 1)
            both = jnp.concatenate([rows, more], axis=0)
            return written(both, norm_parts(both, over_all))[0]

        out = lax.cond(state[1] >= int(FAR), lambda: general(embed_grad, ids), extra)
        return out, jnp.int32(0)

    held, over = send_first(embed_grad, ids)
    rows, over = send_on(held, over, 0)
    out, short = written(rows, norm_parts(rows, over))
    out, _ = lax.while_loop(lambda state: state[1] > 0, again, (out, short[0]))
    return out.T


def solution(mesh):
    torus = Mesh(mesh.devices.reshape(8, 4, 3, 4, 2), AXES)
    return jax.shard_map(
        per_device,
        mesh=torus,
        in_specs=(P(DP, PIPE), P(DP)),
        out_specs=P(DP, PIPE),
        check_vma=False,
    )
```

```python
import functools
import math

import jax
import jax.numpy as jnp
from jax import lax
from jax.experimental import pallas as pl
from jax.experimental.pallas import tpu as pltpu
from jax.sharding import Mesh
from jax.sharding import PartitionSpec as P

D = 4608
VOC_DEV = 1408
WIDE = 640
TAIL = 512
AUX = 64
Y, X, ZH, ZL, CORE = AXES = ("dp_0", "dp_1", "dp_2", "pipe_0", "pipe_1")
DP = AXES[:3]
PIPE = AXES[3:]
F32 = jnp.float32
BF16 = jnp.bfloat16

FIRST = (Y,)
FIRST_CAP = 24
SECOND = (X, ZH)
SECOND_CAP = 16
FAR = 4096.0
NORM_1 = (ZH, ZL, CORE)
NORM_2 = (Y, X)


def axis_size(axes):
    return math.prod({Y: 8, X: 4, ZH: 3, ZL: 4, CORE: 2}[a] for a in axes)


def floor_div(value, by):
    return jnp.floor((value + 0.5) * (1.0 / by))


def place(code, axes):
    y = floor_div(code - 1.0, 12 * VOC_DEV)
    rest = code - 1.0 - y * (12 * VOC_DEV)
    x = floor_div(rest, 3 * VOC_DEV)
    zh = floor_div(rest - x * (3 * VOC_DEV), VOC_DEV)
    index = 0.0
    for axis in axes:
        index = index * axis_size((axis,)) + {Y: y, X: x, ZH: zh}[axis]
    return index


def square_iota(n):
    return (lax.broadcasted_iota(jnp.int32, (n, n), 0), lax.broadcasted_iota(jnp.int32, (n, n), 1))


def column_to_row(column):
    i, j = square_iota(column.shape[0])
    return jnp.sum(jnp.where(i == j, column, 0.0), axis=0, keepdims=True)


def row_to_column(row):
    i, j = square_iota(row.shape[1])
    return jnp.sum(jnp.where(i == j, row, 0.0), axis=1, keepdims=True)


def decode(tail):
    lane = lax.broadcasted_iota(jnp.int32, (1, 128), 1)
    weight = jnp.where(lane == AUX, 1024.0, jnp.where(lane == AUX + 1, 8.0, jnp.where(lane == AUX + 2, 1.0, 0.0)))
    return jnp.sum(tail.astype(F32) * weight, axis=1, keepdims=True)


def encode(code):
    high = jnp.floor(code * (1.0 / 1024))
    rest = code - high * 1024.0
    middle = jnp.floor(rest * (1.0 / 8))
    low = rest - middle * 8.0
    lane = lax.broadcasted_iota(jnp.int32, (1, 128), 1)
    return jnp.where(lane == AUX, high, jnp.where(lane == AUX + 1, middle, jnp.where(lane == AUX + 2, low, 0.0)))


def pack(code_row, code_col, axes):
    n = code_row.shape[1]
    i, j = square_iota(n)
    real_row = code_row > 0.5
    real_col = code_col > 0.5
    to_row = jnp.where(real_row, place(code_row, axes), -1.0)
    to_col = jnp.where(real_col, place(code_col, axes), -1.0)
    same = jnp.where((code_col == code_row) & real_row, 1.0, 0.0)
    above = jnp.where(i < j, same, 0.0)
    below = jnp.where(j < i, same, 0.0)
    count_row = jnp.sum(same, axis=0, keepdims=True)
    lead_row = (jnp.sum(above, axis=0, keepdims=True) == 0.0) & real_row
    lead_col = (jnp.sum(below, axis=1, keepdims=True) == 0.0) & real_col
    width_row = jnp.where(lead_row, jnp.minimum(count_row, 2.0), 0.0)
    before = jnp.sum(jnp.where((to_col == to_row) & (j < i), width_row, 0.0), axis=1, keepdims=True)
    before = jnp.where(lead_col, before, 0.0)
    slot_in = jnp.sum(same * before, axis=0, keepdims=True)
    most = jnp.max(jnp.where(real_row, slot_in + jnp.minimum(count_row, 2.0), 0.0), axis=1, keepdims=True)
    return to_row, slot_in, count_row, lead_row, most


def fill(out_ref, where, cap, turn, code_row, head, tail):
    to_row, slot_in, count_row, lead_row, _ = where
    slots = out_ref.shape[0]
    slot = lax.broadcasted_iota(jnp.int32, (slots, to_row.shape[1]), 0).astype(F32)
    slot_in = slot_in - float(turn * cap)

    def at(place_in, valid):
        fits = valid & (to_row > -0.5) & (place_in > -0.5) & (place_in < cap - 0.5)
        return slot == jnp.where(fits, to_row * cap + place_in, -1.0)

    first = at(slot_in, True)
    second = at(slot_in + 1.0, count_row > 1.5)
    take = jnp.where(first | second, 1.0, 0.0)
    code = jnp.sum(jnp.where(lead_row, take * code_row, 0.0), axis=1, keepdims=True)
    is_second = jnp.max(jnp.where(second, 1.0, 0.0), axis=1, keepdims=True) > 0.5
    take = take.astype(BF16)

    def split(rows):
        total = jnp.dot(take, rows, preferred_element_type=F32)
        kept = total.astype(BF16).astype(F32)
        return jnp.where(is_second, total - kept, kept)

    out_ref[:, :TAIL] = split(head).astype(BF16)
    lane = lax.broadcasted_iota(jnp.int32, (1, 128), 1)
    out_ref[:, TAIL:] = jnp.where(lane < AUX, split(tail), encode(code)).astype(BF16)


def first_kernel(grad_hbm, ids_hbm, out_ref, over_ref, grad_ref, ids_ref, sems):
    load_ids = pltpu.make_async_copy(ids_hbm, ids_ref, sems.at[0])
    load = pltpu.make_async_copy(grad_hbm, grad_ref, sems.at[1])
    load_ids.start()
    load.start()
    load_ids.wait()
    code_row = ids_ref[...].astype(F32) + 1.0
    code_col = row_to_column(code_row)
    where = pack(code_row, code_col, FIRST)
    over_ref[...] = jnp.broadcast_to(jnp.where(where[-1] > FIRST_CAP, FAR, 0.0), over_ref.shape)
    load.wait()
    tail = grad_ref[:, TAIL:]
    tail = jnp.concatenate([tail, jnp.zeros_like(tail)], axis=1)
    fill(out_ref, where, FIRST_CAP, 0, code_row, grad_ref[:, :TAIL], tail)


def second_kernel(rows_ref, over_in_ref, out_ref, over_ref, *, turn):
    tail = rows_ref[:, TAIL:]
    code_col = decode(tail)
    code_row = column_to_row(code_col)
    where = pack(code_row, code_col, SECOND)
    fill(out_ref, where, SECOND_CAP, turn, code_row, rows_ref[:, :TAIL], tail)
    more = where[-1]
    over = jnp.where(more > 2 * SECOND_CAP, FAR, jnp.where(more > SECOND_CAP, 1.0, 0.0))
    over_ref[...] = jnp.broadcast_to(over, over_ref.shape) + over_in_ref[...]


def features(rows_ref):
    lane = lax.broadcasted_iota(jnp.int32, (1, 128), 1)
    tail = rows_ref[:, TAIL:]
    return rows_ref[:, :TAIL], jnp.where(lane < AUX, tail.astype(F32), 0.0).astype(BF16)


def norm_kernel(rows_ref, over_ref, part_ref):
    code_col = decode(rows_ref[:, TAIL:])
    code_row = column_to_row(code_col)
    head, tail = features(rows_ref)
    nt = (((1,), (1,)), ((), ()))
    gram = lax.dot_general(head, head, nt, preferred_element_type=F32)
    gram = gram + lax.dot_general(tail, tail, nt, preferred_element_type=F32)
    gram = jnp.where((code_col == code_row) & (code_row > 0.5), gram, 0.0)
    squares = jnp.sum(jnp.sum(gram, axis=0, keepdims=True), axis=1, keepdims=True)
    lane = lax.broadcasted_iota(jnp.int32, (1, 128), 1)
    part = jnp.where(lane == 0, squares, jnp.where(lane == 1, over_ref[:1, :], 0.0))
    part_ref[...] = jnp.broadcast_to(part[:, None, :], part_ref.shape)


def clip_factor(total, tokens):
    grad_norm = jnp.sqrt(total * float(D) + 1e-06)
    return jnp.minimum(1.0, 0.2 * math.sqrt(tokens * D) / grad_norm)


def relay_kernel(parts_ref, out_ref):
    out_ref[...] = jnp.broadcast_to(jnp.sum(parts_ref[...], axis=0, keepdims=True), out_ref.shape)


EDGES = (0, 256, 512, 768, 1024, 1280, VOC_DEV)


def write_kernel(rows_ref, parts_ref, out_hbm, short_hbm, made_ref, short_ref, sems, *, tokens):
    turned = rows_ref[...].T[: made_ref.shape[0], :]
    lane = lax.broadcasted_iota(jnp.int32, (1, 128), 1)
    parts = jnp.sum(parts_ref[...], axis=0)
    total = jnp.sum(jnp.where(lane == 0, parts, 0.0), axis=1, keepdims=True)
    short_ref[0] = jnp.max(jnp.where(lane == 1, parts, 0.0)).astype(jnp.int32)
    copies = [pltpu.make_async_copy(short_ref, short_hbm, sems.at[len(EDGES) - 1])]
    copies[0].start()
    scale = clip_factor(total, tokens) * math.sqrt(D)
    code = decode(rows_ref[:, TAIL:])
    local = code - 1.0
    local = jnp.where(code > 0.5, local - VOC_DEV * floor_div(local, VOC_DEV), -1.0).astype(jnp.int32)
    for k, (low, high) in enumerate(zip(EDGES[:-1], EDGES[1:])):
        here = lax.broadcasted_iota(jnp.int32, (local.shape[0], high - low), 1) + low
        pick = jnp.where(here == local, 1.0, 0.0).astype(BF16)
        made_ref[:, low:high] = jnp.dot(turned, pick, preferred_element_type=F32) * scale
        copies.append(pltpu.make_async_copy(made_ref.at[:, low:high], out_hbm.at[:, low:high], sems.at[k]))
        copies[-1].start()
    for copy in copies:
        copy.wait()


def shape(rows, cols, dtype=F32):
    return jax.ShapeDtypeStruct((rows, cols), dtype)


def near(dims, dtype=F32):
    return pltpu.VMEM(dims, dtype)


def times_kernel(sums_ref, scale_ref, out_ref):
    out_ref[...] = sums_ref[...] * scale_ref[...]


def around(axes, sizes, value, body, init):
    if not axes:
        return value, body(value, init)
    axis, n = axes[0], sizes[0]
    ring = [(k, (k + 1) % n) for k in range(n)]

    def step(_, carry):
        held, acc = around(axes[1:], sizes[1:], carry[0], body, carry[1])
        return jax.tree.map(lambda a: lax.ppermute(a, axis, ring), held), acc

    return lax.fori_loop(0, n, step, (value, init))


def general(embed_grad, ids):
    tokens = ids.shape[0]
    offset = lax.axis_index(DP) * VOC_DEV

    def add(held, acc):
        rows, names = held
        here = lax.broadcasted_iota(jnp.int32, (VOC_DEV, tokens), 0)
        pick = (here == (names[0] - offset)[None, :]).astype(BF16)
        return acc + jnp.dot(pick, rows, preferred_element_type=F32)

    names = jnp.broadcast_to(ids[None, :], (8, tokens))
    cols = embed_grad.shape[1]
    padded = jnp.pad(embed_grad, ((0, 0), (0, WIDE - cols)))
    _, summed = around(DP, (8, 4, 3), (padded, names), add, jnp.zeros((VOC_DEV, WIDE), F32))
    summed = summed[:, :cols]
    total = jnp.sum(summed * summed)
    for axis in AXES:
        total = lax.psum(total, axis)
    scale = clip_factor(total, tokens * 96) * math.sqrt(D)
    return pl.pallas_call(times_kernel, out_shape=shape(cols, VOC_DEV), name="times")(summed.T, scale.reshape(1, 1))


def kernel(body, out_shape, name, **more):
    vmem = pl.BlockSpec(memory_space=pltpu.VMEM)

    def call(*arrays):
        held = [pltpu.with_memory_space_constraint(a, pltpu.VMEM) for a in arrays]
        return pl.pallas_call(body, in_specs=[vmem] * len(held), out_shape=out_shape, name=name, **more)(*held)

    return call


def send_on(held, over, turn):
    slots = axis_size(SECOND) * SECOND_CAP
    body = functools.partial(second_kernel, turn=turn)
    sent, over = kernel(body, (near((slots, WIDE), BF16), near((8, 128))), "second")(held, over)
    return lax.all_to_all(sent, SECOND, 0, 0, tiled=True), over


def norm_parts(rows, over):
    n1, n2 = axis_size(NORM_1), axis_size(NORM_2)
    part = kernel(norm_kernel, near((n1, 1, 128)), "squares")(rows, over)
    part = lax.all_to_all(part, NORM_1, 0, 0, tiled=True)
    part = kernel(relay_kernel, near((n2, 1, 128)), "relay")(part)
    return lax.all_to_all(part, NORM_2, 0, 0, tiled=True)


def send_first(embed_grad, ids):
    tokens, cols = embed_grad.shape
    slots_1 = axis_size(FIRST) * FIRST_CAP
    hbm = pl.BlockSpec(memory_space=pltpu.HBM)
    sent, over = pl.pallas_call(
        first_kernel,
        in_specs=[hbm, hbm],
        out_shape=(near((slots_1, WIDE), BF16), near((8, 128))),
        scratch_shapes=[
            pltpu.VMEM((tokens, cols), BF16),
            pltpu.VMEM((1, tokens), jnp.int32),
            pltpu.SemaphoreType.DMA((2,)),
        ],
        name="first",
    )(*[pltpu.with_memory_space_constraint(a, pltpu.HBM) for a in (embed_grad, ids.reshape(1, tokens))])
    return lax.all_to_all(sent, FIRST, 0, 0, tiled=True), over


def per_device(embed_grad, ids):
    tokens, cols = embed_grad.shape

    def written(rows, parts):
        return kernel(
            functools.partial(write_kernel, tokens=tokens * 96),
            (shape(cols, VOC_DEV), jax.ShapeDtypeStruct((1,), jnp.int32)),
            "rows",
            out_specs=(pl.BlockSpec(memory_space=pltpu.HBM),) * 2,
            scratch_shapes=[
                pltpu.VMEM((cols, VOC_DEV), F32),
                pltpu.SMEM((1,), jnp.int32),
                pltpu.SemaphoreType.DMA((len(EDGES),)),
            ],
        )(rows, parts)

    def again(state):
        def extra():
            held, over = send_first(embed_grad, ids)
            rows, over_all = send_on(held, over, 0)
            more, _ = send_on(held, over, 1)
            both = jnp.concatenate([rows, more], axis=0)
            return written(both, norm_parts(both, over_all))[0]

        out = lax.cond(state[1] >= int(FAR), lambda: general(embed_grad, ids), extra)
        return out, jnp.int32(0)

    held, over = send_first(embed_grad, ids)
    rows, over = send_on(held, over, 0)
    out, short = written(rows, norm_parts(rows, over))
    out, _ = lax.while_loop(lambda state: state[1] > 0, again, (out, short[0]))
    return out.T


def solution(mesh):
    torus = Mesh(mesh.devices.reshape(8, 4, 3, 4, 2), AXES)
    return jax.shard_map(
        per_device,
        mesh=torus,
        in_specs=(P(DP, PIPE), P(DP)),
        out_specs=P(DP, PIPE),
        check_vma=False,
    )
```

```python
import functools
import math

import jax
import jax.numpy as jnp
from jax import lax
from jax.experimental import pallas as pl
from jax.experimental.pallas import tpu as pltpu
from jax.sharding import Mesh
from jax.sharding import PartitionSpec as P

D = 4608
VOC_DEV = 1408
WIDE = 640
TAIL = 512
AUX = 64
Y, X, ZH, ZL, CORE = AXES = ("dp_0", "dp_1", "dp_2", "pipe_0", "pipe_1")
DP = AXES[:3]
PIPE = AXES[3:]
F32 = jnp.float32
BF16 = jnp.bfloat16

FIRST = (Y,)
FIRST_CAP = 24
SECOND = (X, ZH)
SECOND_CAP = 16
FAR = 4096.0
NORM_1 = (ZH, ZL, CORE)
NORM_2 = (Y, X)


def axis_size(axes):
    return math.prod({Y: 8, X: 4, ZH: 3, ZL: 4, CORE: 2}[a] for a in axes)


def floor_div(value, by):
    return jnp.floor((value + 0.5) * (1.0 / by))


def place(code, axes):
    y = floor_div(code - 1.0, 12 * VOC_DEV)
    rest = code - 1.0 - y * (12 * VOC_DEV)
    x = floor_div(rest, 3 * VOC_DEV)
    zh = floor_div(rest - x * (3 * VOC_DEV), VOC_DEV)
    index = 0.0
    for axis in axes:
        index = index * axis_size((axis,)) + {Y: y, X: x, ZH: zh}[axis]
    return index


def square_iota(n):
    return (lax.broadcasted_iota(jnp.int32, (n, n), 0), lax.broadcasted_iota(jnp.int32, (n, n), 1))


def column_to_row(column):
    i, j = square_iota(column.shape[0])
    return jnp.sum(jnp.where(i == j, column, 0.0), axis=0, keepdims=True)


def row_to_column(row):
    i, j = square_iota(row.shape[1])
    return jnp.sum(jnp.where(i == j, row, 0.0), axis=1, keepdims=True)


def decode(tail):
    lane = lax.broadcasted_iota(jnp.int32, (1, 128), 1)
    weight = jnp.where(lane == AUX, 1024.0, jnp.where(lane == AUX + 1, 8.0, jnp.where(lane == AUX + 2, 1.0, 0.0)))
    return jnp.sum(tail.astype(F32) * weight, axis=1, keepdims=True)


def encode(code):
    high = jnp.floor(code * (1.0 / 1024))
    rest = code - high * 1024.0
    middle = jnp.floor(rest * (1.0 / 8))
    low = rest - middle * 8.0
    lane = lax.broadcasted_iota(jnp.int32, (1, 128), 1)
    return jnp.where(lane == AUX, high, jnp.where(lane == AUX + 1, middle, jnp.where(lane == AUX + 2, low, 0.0)))


def pack(code_row, code_col, axes):
    n = code_row.shape[1]
    i, j = square_iota(n)
    real_row = code_row > 0.5
    real_col = code_col > 0.5
    to_row = jnp.where(real_row, place(code_row, axes), -1.0)
    to_col = jnp.where(real_col, place(code_col, axes), -1.0)
    same = jnp.where((code_col == code_row) & real_row, 1.0, 0.0)
    above = jnp.where(i < j, same, 0.0)
    below = jnp.where(j < i, same, 0.0)
    count_row = jnp.sum(same, axis=0, keepdims=True)
    lead_row = (jnp.sum(above, axis=0, keepdims=True) == 0.0) & real_row
    lead_col = (jnp.sum(below, axis=1, keepdims=True) == 0.0) & real_col
    width_row = jnp.where(lead_row, jnp.minimum(count_row, 2.0), 0.0)
    before = jnp.sum(jnp.where((to_col == to_row) & (j < i), width_row, 0.0), axis=1, keepdims=True)
    before = jnp.where(lead_col, before, 0.0)
    slot_in = jnp.sum(same * before, axis=0, keepdims=True)
    most = jnp.max(jnp.where(real_row, slot_in + jnp.minimum(count_row, 2.0), 0.0), axis=1, keepdims=True)
    return to_row, slot_in, count_row, lead_row, most


def fill(out_ref, where, cap, turn, code_row, head, tail):
    to_row, slot_in, count_row, lead_row, _ = where
    slots = out_ref.shape[0]
    slot = lax.broadcasted_iota(jnp.int32, (slots, to_row.shape[1]), 0).astype(F32)
    slot_in = slot_in - float(turn * cap)

    def at(place_in, valid):
        fits = valid & (to_row > -0.5) & (place_in > -0.5) & (place_in < cap - 0.5)
        return slot == jnp.where(fits, to_row * cap + place_in, -1.0)

    first = at(slot_in, True)
    second = at(slot_in + 1.0, count_row > 1.5)
    take = jnp.where(first | second, 1.0, 0.0)
    code = jnp.sum(jnp.where(lead_row, take * code_row, 0.0), axis=1, keepdims=True)
    is_second = jnp.max(jnp.where(second, 1.0, 0.0), axis=1, keepdims=True) > 0.5
    take = take.astype(BF16)

    def split(rows):
        total = jnp.dot(take, rows, preferred_element_type=F32)
        kept = total.astype(BF16).astype(F32)
        return jnp.where(is_second, total - kept, kept)

    out_ref[:, :TAIL] = split(head).astype(BF16)
    lane = lax.broadcasted_iota(jnp.int32, (1, 128), 1)
    out_ref[:, TAIL:] = jnp.where(lane < AUX, split(tail), encode(code)).astype(BF16)


def first_kernel(grad_hbm, ids_hbm, out_ref, over_ref, grad_ref, ids_ref, sems):
    load_ids = pltpu.make_async_copy(ids_hbm, ids_ref, sems.at[0])
    load = pltpu.make_async_copy(grad_hbm, grad_ref, sems.at[1])
    load_ids.start()
    load.start()
    load_ids.wait()
    code_row = ids_ref[...].astype(F32) + 1.0
    code_col = row_to_column(code_row)
    where = pack(code_row, code_col, FIRST)
    over_ref[...] = jnp.broadcast_to(jnp.where(where[-1] > FIRST_CAP, FAR, 0.0), over_ref.shape)
    load.wait()
    tail = grad_ref[:, TAIL:]
    tail = jnp.concatenate([tail, jnp.zeros_like(tail)], axis=1)
    fill(out_ref, where, FIRST_CAP, 0, code_row, grad_ref[:, :TAIL], tail)


def second_kernel(rows_ref, over_in_ref, out_ref, over_ref, *, turn):
    tail = rows_ref[:, TAIL:]
    code_col = decode(tail)
    code_row = column_to_row(code_col)
    where = pack(code_row, code_col, SECOND)
    fill(out_ref, where, SECOND_CAP, turn, code_row, rows_ref[:, :TAIL], tail)
    more = where[-1]
    over = jnp.where(more > 2 * SECOND_CAP, FAR, jnp.where(more > SECOND_CAP, 1.0, 0.0))
    over_ref[...] = jnp.broadcast_to(over, over_ref.shape) + over_in_ref[...]


def features(rows_ref):
    lane = lax.broadcasted_iota(jnp.int32, (1, 128), 1)
    tail = rows_ref[:, TAIL:]
    return rows_ref[:, :TAIL], jnp.where(lane < AUX, tail.astype(F32), 0.0).astype(BF16)


def norm_kernel(rows_ref, over_ref, part_ref):
    code_col = decode(rows_ref[:, TAIL:])
    code_row = column_to_row(code_col)
    head, tail = features(rows_ref)
    nt = (((1,), (1,)), ((), ()))
    gram = lax.dot_general(head, head, nt, preferred_element_type=F32)
    gram = gram + lax.dot_general(tail, tail, nt, preferred_element_type=F32)
    gram = jnp.where((code_col == code_row) & (code_row > 0.5), gram, 0.0)
    squares = jnp.sum(jnp.sum(gram, axis=0, keepdims=True), axis=1, keepdims=True)
    lane = lax.broadcasted_iota(jnp.int32, (1, 128), 1)
    part = jnp.where(lane == 0, squares, jnp.where(lane == 1, over_ref[:1, :], 0.0))
    part_ref[...] = jnp.broadcast_to(part[:, None, :], part_ref.shape)


def clip_factor(total, tokens):
    grad_norm = jnp.sqrt(total * float(D) + 1e-06)
    return jnp.minimum(1.0, 0.2 * math.sqrt(tokens * D) / grad_norm)


def relay_kernel(parts_ref, out_ref):
    out_ref[...] = jnp.broadcast_to(jnp.sum(parts_ref[...], axis=0, keepdims=True), out_ref.shape)


EDGES = (0, 256, 512, 768, 1024, 1280, VOC_DEV)


def prepare_kernel(rows_ref, turned_ref, pick_ref):
    turned_ref[...] = rows_ref[...].T[: turned_ref.shape[0], :]
    code = decode(rows_ref[:, TAIL:])
    local = code - 1.0
    local = jnp.where(code > 0.5, local - VOC_DEV * floor_div(local, VOC_DEV), -1.0).astype(jnp.int32)
    here = lax.broadcasted_iota(jnp.int32, pick_ref.shape, 1)
    pick_ref[...] = jnp.where(here == local, 1.0, 0.0).astype(BF16)


def write_kernel(turned_ref, pick_ref, parts_ref, out_hbm, short_hbm, made_ref, short_ref, sems, *, tokens):
    lane = lax.broadcasted_iota(jnp.int32, (1, 128), 1)
    parts = jnp.sum(parts_ref[...], axis=0)
    total = jnp.sum(jnp.where(lane == 0, parts, 0.0), axis=1, keepdims=True)
    short_ref[0] = jnp.max(jnp.where(lane == 1, parts, 0.0)).astype(jnp.int32)
    copies = [pltpu.make_async_copy(short_ref, short_hbm, sems.at[len(EDGES) - 1])]
    copies[0].start()
    scale = clip_factor(total, tokens) * math.sqrt(D)
    for k, (low, high) in enumerate(zip(EDGES[:-1], EDGES[1:])):
        made_ref[:, low:high] = jnp.dot(turned_ref[...], pick_ref[:, low:high], preferred_element_type=F32) * scale
        copies.append(pltpu.make_async_copy(made_ref.at[:, low:high], out_hbm.at[:, low:high], sems.at[k]))
        copies[-1].start()
    for copy in copies:
        copy.wait()


def shape(rows, cols, dtype=F32):
    return jax.ShapeDtypeStruct((rows, cols), dtype)


def near(dims, dtype=F32):
    return pltpu.VMEM(dims, dtype)


def times_kernel(sums_ref, scale_ref, out_ref):
    out_ref[...] = sums_ref[...] * scale_ref[...]


def around(axes, sizes, value, body, init):
    if not axes:
        return value, body(value, init)
    axis, n = axes[0], sizes[0]
    ring = [(k, (k + 1) % n) for k in range(n)]

    def step(_, carry):
        held, acc = around(axes[1:], sizes[1:], carry[0], body, carry[1])
        return jax.tree.map(lambda a: lax.ppermute(a, axis, ring), held), acc

    return lax.fori_loop(0, n, step, (value, init))


def general(embed_grad, ids):
    tokens = ids.shape[0]
    offset = lax.axis_index(DP) * VOC_DEV

    def add(held, acc):
        rows, names = held
        here = lax.broadcasted_iota(jnp.int32, (VOC_DEV, tokens), 0)
        pick = (here == (names[0] - offset)[None, :]).astype(BF16)
        return acc + jnp.dot(pick, rows, preferred_element_type=F32)

    names = jnp.broadcast_to(ids[None, :], (8, tokens))
    cols = embed_grad.shape[1]
    padded = jnp.pad(embed_grad, ((0, 0), (0, WIDE - cols)))
    _, summed = around(DP, (8, 4, 3), (padded, names), add, jnp.zeros((VOC_DEV, WIDE), F32))
    summed = summed[:, :cols]
    total = jnp.sum(summed * summed)
    for axis in AXES:
        total = lax.psum(total, axis)
    scale = clip_factor(total, tokens * 96) * math.sqrt(D)
    return pl.pallas_call(times_kernel, out_shape=shape(cols, VOC_DEV), name="times")(summed.T, scale.reshape(1, 1))


def kernel(body, out_shape, name, **more):
    vmem = pl.BlockSpec(memory_space=pltpu.VMEM)

    def call(*arrays):
        held = [pltpu.with_memory_space_constraint(a, pltpu.VMEM) for a in arrays]
        return pl.pallas_call(body, in_specs=[vmem] * len(held), out_shape=out_shape, name=name, **more)(*held)

    return call


def send_on(held, over, turn):
    slots = axis_size(SECOND) * SECOND_CAP
    body = functools.partial(second_kernel, turn=turn)
    sent, over = kernel(body, (near((slots, WIDE), BF16), near((8, 128))), "second")(held, over)
    return lax.all_to_all(sent, SECOND, 0, 0, tiled=True), over


def norm_parts(rows, over):
    n1, n2 = axis_size(NORM_1), axis_size(NORM_2)
    part = kernel(norm_kernel, near((n1, 1, 128)), "squares")(rows, over)
    part = lax.all_to_all(part, NORM_1, 0, 0, tiled=True)
    part = kernel(relay_kernel, near((n2, 1, 128)), "relay")(part)
    return lax.all_to_all(part, NORM_2, 0, 0, tiled=True)


def send_first(embed_grad, ids):
    tokens, cols = embed_grad.shape
    slots_1 = axis_size(FIRST) * FIRST_CAP
    hbm = pl.BlockSpec(memory_space=pltpu.HBM)
    sent, over = pl.pallas_call(
        first_kernel,
        in_specs=[hbm, hbm],
        out_shape=(near((slots_1, WIDE), BF16), near((8, 128))),
        scratch_shapes=[
            pltpu.VMEM((tokens, cols), BF16),
            pltpu.VMEM((1, tokens), jnp.int32),
            pltpu.SemaphoreType.DMA((2,)),
        ],
        name="first",
    )(*[pltpu.with_memory_space_constraint(a, pltpu.HBM) for a in (embed_grad, ids.reshape(1, tokens))])
    return lax.all_to_all(sent, FIRST, 0, 0, tiled=True), over


def per_device(embed_grad, ids):
    tokens, cols = embed_grad.shape

    def written(rows, parts):
        slots = rows.shape[0]
        made = kernel(prepare_kernel, (near((cols, slots), BF16), near((slots, VOC_DEV), BF16)), "prepare")(rows)
        return kernel(
            functools.partial(write_kernel, tokens=tokens * 96),
            (shape(cols, VOC_DEV), jax.ShapeDtypeStruct((1,), jnp.int32)),
            "rows",
            out_specs=(pl.BlockSpec(memory_space=pltpu.HBM),) * 2,
            scratch_shapes=[
                pltpu.VMEM((cols, VOC_DEV), F32),
                pltpu.SMEM((1,), jnp.int32),
                pltpu.SemaphoreType.DMA((len(EDGES),)),
            ],
        )(*made, parts)

    def again(state):
        def extra():
            held, over = send_first(embed_grad, ids)
            rows, over_all = send_on(held, over, 0)
            more, _ = send_on(held, over, 1)
            both = jnp.concatenate([rows, more], axis=0)
            return written(both, norm_parts(both, over_all))[0]

        out = lax.cond(state[1] >= int(FAR), lambda: general(embed_grad, ids), extra)
        return out, jnp.int32(0)

    held, over = send_first(embed_grad, ids)
    rows, over = send_on(held, over, 0)
    out, short = written(rows, norm_parts(rows, over))
    out, _ = lax.while_loop(lambda state: state[1] > 0, again, (out, short[0]))
    return out.T


def solution(mesh):
    torus = Mesh(mesh.devices.reshape(8, 4, 3, 4, 2), AXES)
    return jax.shard_map(
        per_device,
        mesh=torus,
        in_specs=(P(DP, PIPE), P(DP)),
        out_specs=P(DP, PIPE),
        check_vma=False,
    )
```

```python
import functools
import math

import jax
import jax.numpy as jnp
from jax import lax
from jax.experimental import pallas as pl
from jax.experimental.pallas import tpu as pltpu
from jax.sharding import Mesh
from jax.sharding import PartitionSpec as P

D = 4608
VOC_DEV = 1408
WIDE = 640
TAIL = 512
AUX = 64
Y, X, ZH, ZL, CORE = AXES = ("dp_0", "dp_1", "dp_2", "pipe_0", "pipe_1")
DP = AXES[:3]
PIPE = AXES[3:]
F32 = jnp.float32
BF16 = jnp.bfloat16

FIRST = (X,)
FIRST_CAP = 32
SECOND = (Y, ZH)
SECOND_CAP = 16
FAR = 4096.0
NORM_1 = (ZH, ZL, CORE)
NORM_2 = (Y, X)


def axis_size(axes):
    return math.prod({Y: 8, X: 4, ZH: 3, ZL: 4, CORE: 2}[a] for a in axes)


def floor_div(value, by):
    return jnp.floor((value + 0.5) * (1.0 / by))


def place(code, axes):
    y = floor_div(code - 1.0, 12 * VOC_DEV)
    rest = code - 1.0 - y * (12 * VOC_DEV)
    x = floor_div(rest, 3 * VOC_DEV)
    zh = floor_div(rest - x * (3 * VOC_DEV), VOC_DEV)
    index = 0.0
    for axis in axes:
        index = index * axis_size((axis,)) + {Y: y, X: x, ZH: zh}[axis]
    return index


def square_iota(n):
    return (lax.broadcasted_iota(jnp.int32, (n, n), 0), lax.broadcasted_iota(jnp.int32, (n, n), 1))


def column_to_row(column):
    i, j = square_iota(column.shape[0])
    return jnp.sum(jnp.where(i == j, column, 0.0), axis=0, keepdims=True)


def row_to_column(row):
    i, j = square_iota(row.shape[1])
    return jnp.sum(jnp.where(i == j, row, 0.0), axis=1, keepdims=True)


def decode(tail):
    lane = lax.broadcasted_iota(jnp.int32, (1, 128), 1)
    weight = jnp.where(lane == AUX, 1024.0, jnp.where(lane == AUX + 1, 8.0, jnp.where(lane == AUX + 2, 1.0, 0.0)))
    return jnp.sum(tail.astype(F32) * weight, axis=1, keepdims=True)


def encode(code):
    high = jnp.floor(code * (1.0 / 1024))
    rest = code - high * 1024.0
    middle = jnp.floor(rest * (1.0 / 8))
    low = rest - middle * 8.0
    lane = lax.broadcasted_iota(jnp.int32, (1, 128), 1)
    return jnp.where(lane == AUX, high, jnp.where(lane == AUX + 1, middle, jnp.where(lane == AUX + 2, low, 0.0)))


def pack(code_row, code_col, axes):
    n = code_row.shape[1]
    i, j = square_iota(n)
    real_row = code_row > 0.5
    real_col = code_col > 0.5
    to_row = jnp.where(real_row, place(code_row, axes), -1.0)
    to_col = jnp.where(real_col, place(code_col, axes), -1.0)
    same = jnp.where((code_col == code_row) & real_row, 1.0, 0.0)
    above = jnp.where(i < j, same, 0.0)
    below = jnp.where(j < i, same, 0.0)
    count_row = jnp.sum(same, axis=0, keepdims=True)
    lead_row = (jnp.sum(above, axis=0, keepdims=True) == 0.0) & real_row
    lead_col = (jnp.sum(below, axis=1, keepdims=True) == 0.0) & real_col
    width_row = jnp.where(lead_row, jnp.minimum(count_row, 2.0), 0.0)
    before = jnp.sum(jnp.where((to_col == to_row) & (j < i), width_row, 0.0), axis=1, keepdims=True)
    before = jnp.where(lead_col, before, 0.0)
    slot_in = jnp.sum(same * before, axis=0, keepdims=True)
    most = jnp.max(jnp.where(real_row, slot_in + jnp.minimum(count_row, 2.0), 0.0), axis=1, keepdims=True)
    return to_row, slot_in, count_row, lead_row, most


def fill(out_ref, where, cap, turn, code_row, head, tail):
    to_row, slot_in, count_row, lead_row, _ = where
    slots = out_ref.shape[0]
    slot = lax.broadcasted_iota(jnp.int32, (slots, to_row.shape[1]), 0).astype(F32)
    slot_in = slot_in - float(turn * cap)

    def at(place_in, valid):
        fits = valid & (to_row > -0.5) & (place_in > -0.5) & (place_in < cap - 0.5)
        return slot == jnp.where(fits, to_row * cap + place_in, -1.0)

    first = at(slot_in, True)
    second = at(slot_in + 1.0, count_row > 1.5)
    take = jnp.where(first | second, 1.0, 0.0)
    code = jnp.sum(jnp.where(lead_row, take * code_row, 0.0), axis=1, keepdims=True)
    is_second = jnp.max(jnp.where(second, 1.0, 0.0), axis=1, keepdims=True) > 0.5
    take = take.astype(BF16)

    def split(rows):
        total = jnp.dot(take, rows, preferred_element_type=F32)
        kept = total.astype(BF16).astype(F32)
        return jnp.where(is_second, total - kept, kept)

    out_ref[:, :TAIL] = split(head).astype(BF16)
    lane = lax.broadcasted_iota(jnp.int32, (1, 128), 1)
    out_ref[:, TAIL:] = jnp.where(lane < AUX, split(tail), encode(code)).astype(BF16)


def first_kernel(grad_hbm, ids_hbm, out_ref, over_ref, grad_ref, ids_ref, sems):
    load_ids = pltpu.make_async_copy(ids_hbm, ids_ref, sems.at[0])
    load = pltpu.make_async_copy(grad_hbm, grad_ref, sems.at[1])
    load_ids.start()
    load.start()
    load_ids.wait()
    code_row = ids_ref[...].astype(F32) + 1.0
    code_col = row_to_column(code_row)
    where = pack(code_row, code_col, FIRST)
    over_ref[...] = jnp.broadcast_to(jnp.where(where[-1] > FIRST_CAP, FAR, 0.0), over_ref.shape)
    load.wait()
    tail = grad_ref[:, TAIL:]
    tail = jnp.concatenate([tail, jnp.zeros_like(tail)], axis=1)
    fill(out_ref, where, FIRST_CAP, 0, code_row, grad_ref[:, :TAIL], tail)


def second_kernel(rows_ref, over_in_ref, out_ref, over_ref, *, turn):
    tail = rows_ref[:, TAIL:]
    code_col = decode(tail)
    code_row = column_to_row(code_col)
    where = pack(code_row, code_col, SECOND)
    fill(out_ref, where, SECOND_CAP, turn, code_row, rows_ref[:, :TAIL], tail)
    more = where[-1]
    over = jnp.where(more > 2 * SECOND_CAP, FAR, jnp.where(more > SECOND_CAP, 1.0, 0.0))
    over_ref[...] = jnp.broadcast_to(over, over_ref.shape) + over_in_ref[...]


def features(rows_ref):
    lane = lax.broadcasted_iota(jnp.int32, (1, 128), 1)
    tail = rows_ref[:, TAIL:]
    return rows_ref[:, :TAIL], jnp.where(lane < AUX, tail.astype(F32), 0.0).astype(BF16)


def norm_kernel(rows_ref, over_ref, part_ref):
    code_col = decode(rows_ref[:, TAIL:])
    code_row = column_to_row(code_col)
    head, tail = features(rows_ref)
    nt = (((1,), (1,)), ((), ()))
    gram = lax.dot_general(head, head, nt, preferred_element_type=F32)
    gram = gram + lax.dot_general(tail, tail, nt, preferred_element_type=F32)
    gram = jnp.where((code_col == code_row) & (code_row > 0.5), gram, 0.0)
    squares = jnp.sum(jnp.sum(gram, axis=0, keepdims=True), axis=1, keepdims=True)
    lane = lax.broadcasted_iota(jnp.int32, (1, 128), 1)
    part = jnp.where(lane == 0, squares, jnp.where(lane == 1, over_ref[:1, :], 0.0))
    part_ref[...] = jnp.broadcast_to(part[:, None, :], part_ref.shape)


def clip_factor(total, tokens):
    grad_norm = jnp.sqrt(total * float(D) + 1e-06)
    return jnp.minimum(1.0, 0.2 * math.sqrt(tokens * D) / grad_norm)


def relay_kernel(parts_ref, out_ref):
    out_ref[...] = jnp.broadcast_to(jnp.sum(parts_ref[...], axis=0, keepdims=True), out_ref.shape)


EDGES = (0, 256, 512, 768, 1024, 1280, VOC_DEV)


def write_kernel(rows_ref, parts_ref, out_hbm, short_hbm, made_ref, short_ref, sems, *, tokens):
    turned = rows_ref[...].T[: made_ref.shape[0], :]
    lane = lax.broadcasted_iota(jnp.int32, (1, 128), 1)
    parts = jnp.sum(parts_ref[...], axis=0)
    total = jnp.sum(jnp.where(lane == 0, parts, 0.0), axis=1, keepdims=True)
    short_ref[0] = jnp.max(jnp.where(lane == 1, parts, 0.0)).astype(jnp.int32)
    copies = [pltpu.make_async_copy(short_ref, short_hbm, sems.at[len(EDGES) - 1])]
    copies[0].start()
    scale = clip_factor(total, tokens) * math.sqrt(D)
    code = decode(rows_ref[:, TAIL:])
    local = code - 1.0
    local = jnp.where(code > 0.5, local - VOC_DEV * floor_div(local, VOC_DEV), -1.0).astype(jnp.int32)
    for k, (low, high) in enumerate(zip(EDGES[:-1], EDGES[1:])):
        here = lax.broadcasted_iota(jnp.int32, (local.shape[0], high - low), 1) + low
        pick = jnp.where(here == local, 1.0, 0.0).astype(BF16)
        made_ref[:, low:high] = jnp.dot(turned, pick, preferred_element_type=F32) * scale
        copies.append(pltpu.make_async_copy(made_ref.at[:, low:high], out_hbm.at[:, low:high], sems.at[k]))
        copies[-1].start()
    for copy in copies:
        copy.wait()


def shape(rows, cols, dtype=F32):
    return jax.ShapeDtypeStruct((rows, cols), dtype)


def near(dims, dtype=F32):
    return pltpu.VMEM(dims, dtype)


def times_kernel(sums_ref, scale_ref, out_ref):
    out_ref[...] = sums_ref[...] * scale_ref[...]


def around(axes, sizes, value, body, init):
    if not axes:
        return value, body(value, init)
    axis, n = axes[0], sizes[0]
    ring = [(k, (k + 1) % n) for k in range(n)]

    def step(_, carry):
        held, acc = around(axes[1:], sizes[1:], carry[0], body, carry[1])
        return jax.tree.map(lambda a: lax.ppermute(a, axis, ring), held), acc

    return lax.fori_loop(0, n, step, (value, init))


def general(embed_grad, ids):
    tokens = ids.shape[0]
    offset = lax.axis_index(DP) * VOC_DEV

    def add(held, acc):
        rows, names = held
        here = lax.broadcasted_iota(jnp.int32, (VOC_DEV, tokens), 0)
        pick = (here == (names[0] - offset)[None, :]).astype(BF16)
        return acc + jnp.dot(pick, rows, preferred_element_type=F32)

    names = jnp.broadcast_to(ids[None, :], (8, tokens))
    cols = embed_grad.shape[1]
    padded = jnp.pad(embed_grad, ((0, 0), (0, WIDE - cols)))
    _, summed = around(DP, (8, 4, 3), (padded, names), add, jnp.zeros((VOC_DEV, WIDE), F32))
    summed = summed[:, :cols]
    total = jnp.sum(summed * summed)
    for axis in AXES:
        total = lax.psum(total, axis)
    scale = clip_factor(total, tokens * 96) * math.sqrt(D)
    return pl.pallas_call(times_kernel, out_shape=shape(cols, VOC_DEV), name="times")(summed.T, scale.reshape(1, 1))


def kernel(body, out_shape, name, **more):
    vmem = pl.BlockSpec(memory_space=pltpu.VMEM)

    def call(*arrays):
        held = [pltpu.with_memory_space_constraint(a, pltpu.VMEM) for a in arrays]
        return pl.pallas_call(body, in_specs=[vmem] * len(held), out_shape=out_shape, name=name, **more)(*held)

    return call


def send_on(held, over, turn):
    slots = axis_size(SECOND) * SECOND_CAP
    body = functools.partial(second_kernel, turn=turn)
    sent, over = kernel(body, (near((slots, WIDE), BF16), near((8, 128))), "second")(held, over)
    return lax.all_to_all(sent, SECOND, 0, 0, tiled=True), over


def norm_parts(rows, over):
    n1, n2 = axis_size(NORM_1), axis_size(NORM_2)
    part = kernel(norm_kernel, near((n1, 1, 128)), "squares")(rows, over)
    part = lax.all_to_all(part, NORM_1, 0, 0, tiled=True)
    part = kernel(relay_kernel, near((n2, 1, 128)), "relay")(part)
    return lax.all_to_all(part, NORM_2, 0, 0, tiled=True)


def send_first(embed_grad, ids):
    tokens, cols = embed_grad.shape
    slots_1 = axis_size(FIRST) * FIRST_CAP
    hbm = pl.BlockSpec(memory_space=pltpu.HBM)
    sent, over = pl.pallas_call(
        first_kernel,
        in_specs=[hbm, hbm],
        out_shape=(near((slots_1, WIDE), BF16), near((8, 128))),
        scratch_shapes=[
            pltpu.VMEM((tokens, cols), BF16),
            pltpu.VMEM((1, tokens), jnp.int32),
            pltpu.SemaphoreType.DMA((2,)),
        ],
        name="first",
    )(*[pltpu.with_memory_space_constraint(a, pltpu.HBM) for a in (embed_grad, ids.reshape(1, tokens))])
    return lax.all_to_all(sent, FIRST, 0, 0, tiled=True), over


def per_device(embed_grad, ids):
    tokens, cols = embed_grad.shape

    def written(rows, parts):
        return kernel(
            functools.partial(write_kernel, tokens=tokens * 96),
            (shape(cols, VOC_DEV), jax.ShapeDtypeStruct((1,), jnp.int32)),
            "rows",
            out_specs=(pl.BlockSpec(memory_space=pltpu.HBM),) * 2,
            scratch_shapes=[
                pltpu.VMEM((cols, VOC_DEV), F32),
                pltpu.SMEM((1,), jnp.int32),
                pltpu.SemaphoreType.DMA((len(EDGES),)),
            ],
        )(rows, parts)

    def again(state):
        def extra():
            held, over = send_first(embed_grad, ids)
            rows, over_all = send_on(held, over, 0)
            more, _ = send_on(held, over, 1)
            both = jnp.concatenate([rows, more], axis=0)
            return written(both, norm_parts(both, over_all))[0]

        out = lax.cond(state[1] >= int(FAR), lambda: general(embed_grad, ids), extra)
        return out, jnp.int32(0)

    held, over = send_first(embed_grad, ids)
    rows, over = send_on(held, over, 0)
    out, short = written(rows, norm_parts(rows, over))
    out, _ = lax.while_loop(lambda state: state[1] > 0, again, (out, short[0]))
    return out.T


def solution(mesh):
    torus = Mesh(mesh.devices.reshape(8, 4, 3, 4, 2), AXES)
    return jax.shard_map(
        per_device,
        mesh=torus,
        in_specs=(P(DP, PIPE), P(DP)),
        out_specs=P(DP, PIPE),
        check_vma=False,
    )
```
